8 devices in a mesh: nodes: 8 (over z, y, x, core).
Axes of the slice: x: 2, y: 2, z: 1, core: 2. Of those that a mesh axis runs over, the one named last changes fastest.
Arguments:
- adjacency: bfloat16 [16384, 16384], P('nodes')
- features: bfloat16 [16384, 128], P('nodes')
- w_one: float32 [128, 256], replicated
- w_two: float32 [256, 349], replicated
- labels: int32 [16384], P('nodes')
- label_mask: int32 [16384], P('nodes')
Outputs:
- output 1: float32 [], replicated
- output 2: float32 [128, 256], replicated
- output 3: float32 [256, 349], replicated
All inputs are finite; a program needn't handle non-finite values.
Results may differ from the reference program's by a relative error of at most 0.00157.
Values are sent between devices in bfloat16 or wider.
A program may use at most 1 GiB of HBM per device.

```python
import jax
import jax.numpy as jnp
from jax import lax

NUM_NODES = 16384
F_IN = 128
HIDDEN = 256
CLASSES = 349
COMMUNITIES = 8
EDGE_IN = 40
EDGE_OUT = 8
HASH_MOD = 128
HASH_SHIFT = 2048
HASH_RANGE = 32768
LABEL_RATE = 4


def draw_graph(key_base):
    key_mult, key_add, key_comm = jax.random.split(key_base, 3)
    mult_ids = jax.random.randint(key_mult, (NUM_NODES,), 0, HASH_RANGE, dtype=jnp.int32)
    add_ids = jax.random.randint(key_add, (NUM_NODES,), 0, HASH_RANGE, dtype=jnp.int32)
    comm_ids = jax.random.randint(key_comm, (NUM_NODES,), 0, COMMUNITIES, dtype=jnp.int32)
    hashed = (mult_ids[:, None] * mult_ids[None, :] // HASH_SHIFT + add_ids[:, None] + add_ids[None, :]) % HASH_MOD
    edge_limit = jnp.where(comm_ids[:, None] == comm_ids[None, :], EDGE_IN, EDGE_OUT)
    node_ids = jnp.arange(NUM_NODES, dtype=jnp.int32)
    linked = (hashed < edge_limit) | (node_ids[:, None] == node_ids[None, :])
    degree = jnp.sum(linked.astype(jnp.int32), axis=1).astype(jnp.float32)
    inv_root = lax.rsqrt(degree)
    adjacency = jnp.where(linked, inv_root[:, None] * inv_root[None, :], 0.0).astype(jnp.bfloat16)
    return adjacency, jnp.sqrt(jnp.mean(degree))


def draw_mask(key_base):
    key_rate, key_pick = jax.random.split(key_base)
    chosen = jax.random.randint(key_rate, (NUM_NODES,), 0, LABEL_RATE, dtype=jnp.int32) == 0
    forced = jax.random.randint(key_pick, (), 0, NUM_NODES, dtype=jnp.int32)
    return (chosen | (jnp.arange(NUM_NODES, dtype=jnp.int32) == forced)).astype(jnp.int32)


def setup_inputs(seed: int = 0) -> dict:
    key_base = jax.random.key(seed)
    key_graph, key_feat, key_one, key_two, key_label, key_mask = jax.random.split(key_base, 6)
    adjacency, weight_gain = draw_graph(key_graph)
    features = jax.random.normal(key_feat, (NUM_NODES, F_IN), jnp.float32).astype(jnp.bfloat16)
    w_one = jax.random.normal(key_one, (F_IN, HIDDEN), jnp.float32) * (weight_gain * F_IN ** -0.5)
    raw_two = jax.random.normal(key_two, (HIDDEN, CLASSES), jnp.float32)
    w_two = (raw_two - jnp.mean(raw_two, axis=0, keepdims=True)) * (1.5 * weight_gain * HIDDEN ** -0.5)
    labels = jax.random.randint(key_label, (NUM_NODES,), 0, CLASSES, dtype=jnp.int32)
    label_mask = draw_mask(key_mask)
    return {'adjacency': adjacency, 'features': features, 'w_one': w_one, 'w_two': w_two, 'labels': labels, 'label_mask': label_mask}


def contract_rows(left, right):
    return lax.dot_general(left, right, (((0,), (0,)), ((), ())), preferred_element_type=jnp.float32)


def reference(adjacency, features, w_one, w_two, labels, label_mask):
    w_one_b = w_one.astype(jnp.bfloat16)
    w_two_b = w_two.astype(jnp.bfloat16)
    y_one = jnp.dot(features, w_one_b, preferred_element_type=jnp.float32).astype(jnp.bfloat16)
    z_one = jnp.dot(adjacency, y_one, preferred_element_type=jnp.float32)
    h_one = jnp.maximum(z_one, 0.0).astype(jnp.bfloat16)
    y_two = jnp.dot(h_one, w_two_b, preferred_element_type=jnp.float32).astype(jnp.bfloat16)
    z_two = jnp.dot(adjacency, y_two, preferred_element_type=jnp.float32)
    mask_f = label_mask.astype(jnp.float32)
    label_count = jnp.sum(mask_f)
    log_norm = jax.nn.logsumexp(z_two, axis=1)
    onehot = (labels[:, None] == jnp.arange(CLASSES, dtype=jnp.int32)[None, :]).astype(jnp.float32)
    picked = jnp.sum(z_two * onehot, axis=1)
    loss_value = jnp.sum(mask_f * (log_norm - picked)) / label_count
    soft_probs = jnp.exp(z_two - log_norm[:, None])
    g_two = ((soft_probs - onehot) * (mask_f / label_count)[:, None]).astype(jnp.bfloat16)
    grad_y2 = contract_rows(adjacency, g_two).astype(jnp.bfloat16)
    grad_two = contract_rows(h_one, grad_y2)
    grad_h1 = lax.dot_general(grad_y2, w_two_b, (((1,), (1,)), ((), ())), preferred_element_type=jnp.float32)
    grad_z1 = jnp.where(z_one > 0.0, grad_h1, 0.0).astype(jnp.bfloat16)
    grad_y1 = contract_rows(adjacency, grad_z1).astype(jnp.bfloat16)
    grad_one = contract_rows(features, grad_y1)
    return (loss_value, grad_one, grad_two)
```

```python
import jax
import jax.numpy as jnp
from jax import lax
from jax.sharding import PartitionSpec as P


def contract_rows(left, right):
    return lax.dot_general(left, right, (((0,), (0,)), ((), ())), preferred_element_type=jnp.float32)


def mm(left, right):
    return jnp.dot(left, right, preferred_element_type=jnp.float32)


def solution(mesh):
    node_axis = mesh.axis_names[0]

    def gather(x):
        return lax.all_gather(x, node_axis, tiled=True)

    def local_step(adj_rows, feat_rows, w_one, w_two, label_rows, mask_rows):
        classes = w_two.shape[1]
        w_one_b = w_one.astype(jnp.bfloat16)
        w_two_b = w_two.astype(jnp.bfloat16)
        y_one_all = mm(gather(feat_rows), w_one_b).astype(jnp.bfloat16)
        z_one = mm(adj_rows, y_one_all)
        h_one = jnp.maximum(z_one, 0.0).astype(jnp.bfloat16)
        y_two_all = mm(gather(h_one), w_two_b).astype(jnp.bfloat16)
        z_two = mm(adj_rows, y_two_all)
        mask_f = mask_rows.astype(jnp.float32)
        label_count = lax.psum(jnp.sum(mask_f), node_axis)
        log_norm = jax.nn.logsumexp(z_two, axis=1)
        onehot = (label_rows[:, None] == jnp.arange(classes, dtype=jnp.int32)[None, :]).astype(jnp.float32)
        picked = jnp.sum(z_two * onehot, axis=1)
        loss_part = jnp.sum(mask_f * (log_norm - picked))
        soft_probs = jnp.exp(z_two - log_norm[:, None])
        g_two = ((soft_probs - onehot) * (mask_f / label_count)[:, None]).astype(jnp.bfloat16)
        grad_y2 = mm(adj_rows, gather(g_two)).astype(jnp.bfloat16)
        grad_h1 = lax.dot_general(grad_y2, w_two_b, (((1,), (1,)), ((), ())), preferred_element_type=jnp.float32)
        grad_z1 = jnp.where(z_one > 0.0, grad_h1, 0.0).astype(jnp.bfloat16)
        grad_y1 = mm(adj_rows, gather(grad_z1)).astype(jnp.bfloat16)
        loss_sum, grad_one, grad_two = lax.psum(
            (loss_part, contract_rows(feat_rows, grad_y1), contract_rows(h_one, grad_y2)), node_axis)
        return loss_sum / label_count, grad_one, grad_two

    return jax.shard_map(local_step, mesh=mesh, in_specs=(P(node_axis, None), P(node_axis, None), P(None, None), P(None, None), P(node_axis), P(node_axis)), out_specs=(P(), P(None, None), P(None, None)), check_vma=False)
```

```python
import functools

import jax
import jax.numpy as jnp
from jax import lax
from jax.experimental import pallas as pl
from jax.experimental.pallas import tpu as pltpu
from jax.sharding import PartitionSpec as P

MESH = pl.DeviceIdType.MESH
F32, BF16 = jnp.float32, jnp.bfloat16
SLOTS = 4
CHUNK = 512
CHUNKS = 4
ITEMS = 16
LANES = 128


def nt(left, right):
    return lax.dot_general(left, right, (((1,), (1,)), ((), ())), preferred_element_type=F32)


def nn(left, right):
    return jnp.dot(left, right, preferred_element_type=F32)


def gcn_kernel(axis, classes, a_hbm, x_hbm, w1_ref, w2_ref, lab_ref, mask_ref, loss_ref, dw1_ref, dw2_ref,
               ring, xg, hg, gg, dg, acc1, acc2, lhs, e2, w1t, w2t, w2b, cnt, los, mrow,
               s1, s2, ta1, ta2, tc1, tc2, hb1, hb2, tb1, tb2,
               a_sem, x_sem, isend, irecv, dsend, drecv, csend, crecv, lsend, lrecv, rsend, rrecv):
    me = lax.axis_index(axis)
    core, chip = lax.rem(me, 2), lax.div(me, 2)
    cx, cy = lax.rem(chip, 2), lax.div(chip, 2)
    hidden = hg.shape[2]
    rows_p = gg.shape[2]

    def chip_of(m):
        return lax.rem(cy + m // 2, 2) * 2 + lax.rem(cx + m % 2, 2)

    def chip_dyn(m):
        return lax.rem(cy + lax.div(m, 2), 2) * 2 + lax.rem(cx + lax.rem(m, 2), 2)

    partner = chip * 2 + (1 - core)
    to_x, to_y, to_d = (chip_of(m) * 2 + core for m in (1, 2, 3))
    bufs = (xg, hg, gg, dg)

    def rcopy(src, dst, send, recv, dev):
        return pltpu.make_async_remote_copy(src_ref=src, dst_ref=dst, send_sem=send, recv_sem=recv,
                                            device_id=(dev,), device_id_type=MESH)

    def a_copies(i, slot):
        first = chip_dyn(lax.div(i, 4)) * (2 * CHUNK * CHUNKS) + lax.rem(i, 4) * CHUNK
        for h in (0, 1):
            cols = pl.ds(pl.multiple_of(first + h * CHUNK * CHUNKS, CHUNK), CHUNK)
            yield pltpu.make_async_copy(a_hbm.at[:, cols], ring.at[slot, h], a_sem.at[slot, h])

    def own_copies(p, j):
        g, q = bufs[p].at[me, j], p % 2
        return [rcopy(g, g, isend.at[q, 0, j], irecv.at[q, 0, j], to_x),
                rcopy(g, g, isend.at[q, 1, j], irecv.at[q, 1, j], to_y),
                rcopy(g, g, dsend.at[q, 0, j], drecv.at[q, 0, j], partner)]

    def relay_x(p, j):
        g, q, half = bufs[p], p % 2, bufs[p].shape[2] // 2
        g = g.at[to_y, j, pl.ds(0, half)]
        return rcopy(g, g, isend.at[q, 2, j], irecv.at[q, 2, j], to_x)

    def relay_y(p, j):
        g, q, half = bufs[p], p % 2, bufs[p].shape[2] // 2
        g = g.at[to_x, j, pl.ds(half, half)]
        return rcopy(g, g, isend.at[q, 3, j], irecv.at[q, 3, j], to_y)

    def forward(p, m, j):
        g, q = bufs[p].at[chip_of(m) * 2 + core, j], p % 2
        return rcopy(g, g, dsend.at[q, m, j], drecv.at[q, m, j], partner)

    def arrive_xy(p, j):
        q = p % 2
        g = bufs[p].at[to_x, j]
        rcopy(g, g, isend.at[q, 0, j], irecv.at[q, 0, j], to_x).wait_recv()
        relay_y(p, j).start()
        forward(p, 1, j).start()
        g = bufs[p].at[to_y, j]
        rcopy(g, g, isend.at[q, 1, j], irecv.at[q, 1, j], to_y).wait_recv()
        relay_x(p, j).start()
        forward(p, 2, j).start()

    def arrive_d(p, j):
        q, half = p % 2, bufs[p].shape[2] // 2
        g = bufs[p].at[to_d, j, pl.ds(0, half)]
        rcopy(g, g, isend.at[q, 2, j], irecv.at[q, 2, j], to_x).wait_recv()
        g = bufs[p].at[to_d, j, pl.ds(half, half)]
        rcopy(g, g, isend.at[q, 3, j], irecv.at[q, 3, j], to_y).wait_recv()
        forward(p, 3, j).start()

    def arrive_core(p, m, j):
        q = p % 2
        g = bufs[p].at[chip_dyn(m) * 2 + 1 - core, j]
        rcopy(g, g, dsend.at[q, m, j], drecv.at[q, m, j], partner).wait_recv()

    def wait_sends(p, j):
        for copy in own_copies(p, j) + [relay_x(p, j), relay_y(p, j)] + [forward(p, m, j) for m in (1, 2, 3)]:
            copy.wait_send()

    def tile_copies(buf, send, recv):
        for k in range(1, 8):
            yield rcopy(buf.at[me], buf.at[me], send.at[k - 1], recv.at[k - 1], lax.rem(me + k, 8))

    def wait_tiles(buf, send, recv):
        for k, copy in enumerate(tile_copies(buf, send, recv), 1):
            copy.wait_send()
            other = lax.rem(me + 8 - k, 8)
            rcopy(buf.at[other], buf.at[other], send.at[k - 1], recv.at[k - 1], other).wait_recv()

    class Reduce:
        def __init__(self, src, ta, tc, hb, tb, n):
            self.src, self.ta, self.tc, self.hb, self.tb, self.n = src, ta, tc, hb, tb, n
            self.a = rcopy(src.at[1 - core], ta, rsend.at[n, 0], rrecv.at[n, 0], partner)
            self.b1 = [rcopy(hb.at[chip_of(m)], tb.at[m - 1], rsend.at[n, m], rrecv.at[n, m], chip_of(m) * 2 + core)
                       for m in (1, 2, 3)]
            self.b2 = [rcopy(src.at[core, chip], src.at[core, chip], rsend.at[n, 3 + m], rrecv.at[n, 3 + m],
                             chip_of(m) * 2 + core) for m in (1, 2, 3)]
            self.c = rcopy(src.at[core], tc, rsend.at[n, 7], rrecv.at[n, 7], partner)

        def first(self):
            self.a.start()

        def second(self):
            self.a.wait()
            self.hb[...] = self.src[core] + self.ta[...]
            for copy in self.b1:
                copy.start()

        def third(self):
            for copy in self.b1:
                copy.wait()
            self.src[core, chip] = self.hb[chip] + self.tb[0] + self.tb[1] + self.tb[2]
            for copy in self.b2:
                copy.start()

        def fourth(self):
            for m, copy in enumerate(self.b2, 1):
                copy.wait_send()
                g = self.src.at[core, chip_of(m)]
                rcopy(g, g, rsend.at[self.n, 3 + m], rrecv.at[self.n, 3 + m], chip_of(m) * 2 + core).wait_recv()
            self.c.start()

        def last(self, out):
            self.c.wait()
            for k in range(4):
                out[pl.ds(pl.multiple_of(core * 128 + k * 32, 32), 32), :] = self.src[core, k]
                out[pl.ds(pl.multiple_of((1 - core) * 128 + k * 32, 32), 32), :] = self.tc[k]

    reduce1, reduce2 = Reduce(s1, ta1, tc1, hb1, tb1, 0), Reduce(s2, ta2, tc2, hb2, tb2, 1)

    x_copies = [pltpu.make_async_copy(x_hbm.at[j], xg.at[me, j], x_sem.at[j]) for j in range(CHUNKS)]
    for copy in x_copies:
        copy.start()
    for s in range(SLOTS):
        for copy in a_copies(jnp.int32(s), s):
            copy.start()
    cnt[...] = jnp.zeros_like(cnt)
    los[...] = jnp.zeros_like(los)
    cnt[me, 0:1, :] = jnp.sum(mask_ref[...].astype(F32), axis=0)
    barrier = pltpu.get_barrier_semaphore()
    for k in range(1, 8):
        pl.semaphore_signal(barrier, inc=1, device_id=(lax.rem(me + k, 8),), device_id_type=MESH)
    pl.semaphore_wait(barrier, 7)
    for j, copy in enumerate(x_copies):
        copy.wait()
        for send in own_copies(0, j):
            send.start()

    w1t[...] = w1_ref[...].T.astype(BF16)
    w2b[...] = jnp.zeros_like(w2b)
    w2b[:, :classes] = w2_ref[...].astype(BF16)
    w2t[...] = w2b[...].astype(F32).T[:rows_p].astype(BF16)
    e2[:, rows_p:, :] = jnp.zeros((CHUNKS, e2.shape[1] - rows_p, CHUNK), BF16)
    for copy in tile_copies(cnt, csend, crecv):
        copy.start()

    def operands(p, m, j):
        refs = []
        for h in (0, 1):
            dev = chip_dyn(m) * 2 + h
            if p == 0:
                lhs[h, :hidden, :] = nt(w1t[...], xg[dev, j]).astype(BF16)
                refs.append(lhs.at[h, pl.ds(0, hidden)])
            elif p == 1:
                lhs[h] = nn(w2t[...], hg[dev, j]).astype(BF16)
                refs.append(lhs.at[h])
            else:
                refs.append(bufs[p].at[dev, j])
        return refs

    def product(refs, slot, rc):
        rows = pl.ds(rc * CHUNK, CHUNK) if isinstance(rc, int) else pl.ds(pl.multiple_of(rc * CHUNK, CHUNK), CHUNK)
        return nt(refs[0][...], ring[slot, 0, rows, :]) + nt(refs[1][...], ring[slot, 1, rows, :])

    def finish_one(rc):
        z = acc1[rc]
        hg[me, rc] = jnp.maximum(z, 0.0).astype(BF16)

    def finish_two(rc):
        for b in range(CHUNK // LANES):
            lanes = pl.ds(b * LANES, LANES)
            z = acc2[rc, :, lanes]
            index = lax.broadcasted_iota(jnp.int32, z.shape, 0)
            z = jnp.where(index < classes, z, -jnp.inf)
            top = jnp.max(z, axis=0, keepdims=True)
            e = jnp.exp(z - top)
            total = jnp.sum(e, axis=0, keepdims=True)
            hit = index == lab_ref[rc, :, lanes]
            picked = jnp.sum(jnp.where(hit, z, 0.0), axis=0, keepdims=True)
            mask_f = mask_ref[rc, :, lanes].astype(F32)
            los[me, 0:1, lanes] += mask_f * (jnp.log(total) + top - picked)
            onehot = jnp.where(hit, 1.0, 0.0)
            gg[me, rc, :, lanes] = ((e * (1.0 / total) - onehot) * (mask_f / mrow[:, lanes])).astype(BF16)

    def finish_three(rc):
        e2[rc, :rows_p, :] = acc2[rc].astype(BF16)
        dz = nn(w2b[...], e2[rc])
        dg[me, rc] = jnp.where(acc1[rc] > 0.0, dz, 0.0).astype(BF16)

    def finish_four(rc):
        return nn(acc1[rc].astype(BF16), xg[me, rc])

    def phase(p):
        acc = (acc1, acc2, acc2, acc1)[p]

        if p == 1:
            wait_tiles(cnt, csend, crecv)
            total = jnp.sum(jnp.sum(cnt[...], axis=0), axis=0, keepdims=True)
            mrow[...] = jnp.broadcast_to(jnp.sum(total, axis=1, keepdims=True), mrow.shape)
        if p == 3:
            grad = nt(hg[me, 0], e2[0])
            for rc in range(1, CHUNKS):
                grad = grad + nt(hg[me, rc], e2[rc])
            for k in range(8):
                s2[k // 4, k % 4] = grad[k * 32:(k + 1) * 32]
        acc[...] = jnp.zeros_like(acc)
        if p == 2:
            for copy in tile_copies(los, lsend, lrecv):
                copy.start()
        if p == 3:
            reduce2.first()

        def step(i, carry):
            m, j = lax.div(i, 4), lax.rem(i, 4)
            slot = lax.rem(i + p * ITEMS, SLOTS)

            @pl.when((i >= 3) & (i <= 6))
            def _():
                arrive_xy(p, i - 3)

            @pl.when(i >= 11)
            def _():
                arrive_d(p, i - 11)

            if p > 0:
                @pl.when(i < 4)
                def _():
                    wait_sends(p - 1, i)

            if p == 3:
                for at, stage in ((1, reduce2.second), (4, reduce2.third), (7, reduce2.fourth)):
                    pl.when(i == at)(stage)

            arrive_core(p, m, j)
            for copy in a_copies(i, slot):
                copy.wait()
            refs = operands(p, m, j)
            for rc in range(CHUNKS):
                acc[rc] += product(refs, slot, rc)

            def prefetch():
                for copy in a_copies(lax.rem(i + SLOTS, ITEMS), slot):
                    copy.start()

            if p < 3:
                prefetch()
            else:
                pl.when(i + SLOTS < ITEMS)(prefetch)
            return carry

        lax.fori_loop(0, ITEMS - 1, step, 0)

        i = jnp.int32(ITEMS - 1)
        slot = (ITEMS - 1 + p * ITEMS) % SLOTS
        arrive_core(p, jnp.int32(3), CHUNKS - 1)
        for copy in a_copies(i, slot):
            copy.wait()
        refs = operands(p, jnp.int32(3), CHUNKS - 1)

        def finish(rc, carry):
            acc[rc] += product(refs, slot, rc)
            if p < 3:
                (finish_one, finish_two, finish_three)[p](rc)
                for copy in own_copies(p + 1, rc):
                    copy.start()
                return carry
            return carry + finish_four(rc)

        out = lax.fori_loop(0, CHUNKS, finish, jnp.zeros((hidden, LANES), F32) if p == 3 else 0)
        if p < 3:
            for copy in a_copies(jnp.int32((ITEMS - 1 + SLOTS) % ITEMS), slot):
                copy.start()
        return out

    for p in range(4):
        out = phase(p)

    for k in range(8):
        s1[k // 4, k % 4] = out[k * 32:(k + 1) * 32]
    reduce1.first()
    reduce2.last(dw2_ref)
    wait_tiles(los, lsend, lrecv)
    total = jnp.sum(jnp.sum(los[...], axis=0), axis=0, keepdims=True)
    total = jnp.sum(total, axis=1, keepdims=True) / mrow[:, 0:1]
    loss_ref[...] = jnp.broadcast_to(total, loss_ref.shape)
    reduce1.second()
    for j in range(CHUNKS):
        wait_sends(3, j)
    reduce1.third()
    reduce1.fourth()
    reduce1.last(dw1_ref)


def solution(mesh):
    axis = mesh.axis_names[0]

    def local_step(adj_rows, feat_rows, w_one, w_two, label_rows, mask_rows):
        f_in, hidden = w_one.shape
        classes = w_two.shape[1]
        rows_p = -(-classes // 32) * 32
        lanes_p = -(-classes // LANES) * LANES
        rows = adj_rows.shape[0]
        dma = pltpu.SemaphoreType.DMA
        vmem = pl.BlockSpec(memory_space=pltpu.VMEM)
        hbm = pl.BlockSpec(memory_space=pl.ANY)
        loss, dw1, dw2 = pl.pallas_call(
            functools.partial(gcn_kernel, axis, classes),
            name="gcn_step",
            out_shape=(jax.ShapeDtypeStruct((8, LANES), F32), jax.ShapeDtypeStruct((hidden, f_in), F32),
                       jax.ShapeDtypeStruct((hidden, lanes_p), F32)),
            in_specs=[hbm, hbm, vmem, vmem, vmem, vmem],
            out_specs=(vmem, vmem, vmem),
            scratch_shapes=[
                pltpu.VMEM((SLOTS, 2, rows, CHUNK), BF16),
                pltpu.VMEM((8, CHUNKS, CHUNK, f_in), BF16),
                pltpu.VMEM((8, CHUNKS, hidden, CHUNK), BF16),
                pltpu.VMEM((8, CHUNKS, rows_p, CHUNK), BF16),
                pltpu.VMEM((8, CHUNKS, hidden, CHUNK), BF16),
                pltpu.VMEM((CHUNKS, hidden, CHUNK), F32),
                pltpu.VMEM((CHUNKS, rows_p, CHUNK), F32),
                pltpu.VMEM((2, rows_p, CHUNK), BF16),
                pltpu.VMEM((CHUNKS, lanes_p, CHUNK), BF16),
                pltpu.VMEM((hidden, f_in), BF16),
                pltpu.VMEM((rows_p, hidden), BF16),
                pltpu.VMEM((hidden, lanes_p), BF16),
                pltpu.VMEM((8, 8, CHUNK), F32),
                pltpu.VMEM((8, 8, CHUNK), F32),
                pltpu.VMEM((1, CHUNK), F32),
                pltpu.VMEM((2, 4, 32, f_in), F32),
                pltpu.VMEM((2, 4, 32, lanes_p), F32),
                pltpu.VMEM((4, 32, f_in), F32),
                pltpu.VMEM((4, 32, lanes_p), F32),
                pltpu.VMEM((4, 32, f_in), F32),
                pltpu.VMEM((4, 32, lanes_p), F32),
                pltpu.VMEM((4, 32, f_in), F32),
                pltpu.VMEM((4, 32, lanes_p), F32),
                pltpu.VMEM((3, 32, f_in), F32),
                pltpu.VMEM((3, 32, lanes_p), F32),
                dma((SLOTS, 2)), dma((CHUNKS,)),
                dma((2, 4, CHUNKS)), dma((2, 4, CHUNKS)), dma((2, 4, CHUNKS)), dma((2, 4, CHUNKS)),
                dma((7,)), dma((7,)), dma((7,)), dma((7,)), dma((2, 8)), dma((2, 8)),
            ],
            compiler_params=pltpu.CompilerParams(
                collective_id=0, has_side_effects=True, vmem_limit_bytes=67_000_000),
        )(adj_rows, feat_rows.reshape(CHUNKS, CHUNK, f_in), w_one, w_two,
          label_rows.reshape(CHUNKS, 1, CHUNK), mask_rows.reshape(CHUNKS, 1, CHUNK))
        return loss[0, 0], dw1.T, dw2[:, :classes]

    return jax.shard_map(local_step, mesh=mesh, in_specs=(P(axis, None), P(axis, None), P(None, None), P(None, None), P(axis), P(axis)), out_specs=(P(), P(None, None), P(None, None)), check_vma=False)
```

```python
import functools

import jax
import jax.numpy as jnp
from jax import lax
from jax.experimental import pallas as pl
from jax.experimental.pallas import tpu as pltpu
from jax.sharding import PartitionSpec as P

MESH = pl.DeviceIdType.MESH
F32, BF16 = jnp.float32, jnp.bfloat16
SLOTS = 4
CHUNK = 512
CHUNKS = 4
ITEMS = 16
LANES = 128


def nt(left, right):
    return lax.dot_general(left, right, (((1,), (1,)), ((), ())), preferred_element_type=F32)


def nn(left, right):
    return jnp.dot(left, right, preferred_element_type=F32)


def gcn_kernel(axis, classes, a_hbm, x_hbm, w1_hbm, w2_hbm, lab_hbm, mask_hbm, loss_ref, dw1_ref, dw2_ref,
               ring, xg, hg, gg, dg, acc1, acc2, lhs, e2, xt, w1_ref, w2_ref, lab_ref, mask_ref, w1t, w2t, w2b,
               cnt, los, mrow, d1, r1, f1, s2, ta, tc, hb, tb,
               a_sem, x_sem, w_sem, isend, irecv, dsend, drecv, csend, crecv, lsend, lrecv,
               p1send, p1recv, f1send, f1recv, rsend, rrecv):
    me = lax.axis_index(axis)
    core, chip = lax.rem(me, 2), lax.div(me, 2)
    cx, cy = lax.rem(chip, 2), lax.div(chip, 2)
    hidden = hg.shape[2]
    rows_p = gg.shape[2]

    def chip_of(m):
        return lax.rem(cy + m // 2, 2) * 2 + lax.rem(cx + m % 2, 2)

    def chip_dyn(m):
        return lax.rem(cy + lax.div(m, 2), 2) * 2 + lax.rem(cx + lax.rem(m, 2), 2)

    partner = chip * 2 + (1 - core)
    to_x, to_y, to_d = (chip_of(m) * 2 + core for m in (1, 2, 3))
    bufs = (xg, hg, gg, dg)

    def rcopy(src, dst, send, recv, dev):
        return pltpu.make_async_remote_copy(src_ref=src, dst_ref=dst, send_sem=send, recv_sem=recv,
                                            device_id=(dev,), device_id_type=MESH)

    def item(i):
        side = lax.div(lax.rem(i + 4, 16), 8)
        t = lax.rem(i + 12, 16)
        m = side * (1 + lax.rem(t, 2)) + 3 * lax.div(i, 12)
        j = side * lax.div(t, 2) + (1 - side) * lax.rem(i, 4)
        return m, j

    def a_copies(i, slot):
        m, j = item(i)
        first = chip_dyn(m) * (2 * CHUNK * CHUNKS) + j * CHUNK
        for h in (0, 1):
            cols = pl.ds(pl.multiple_of(first + h * CHUNK * CHUNKS, CHUNK), CHUNK)
            yield pltpu.make_async_copy(a_hbm.at[:, cols], ring.at[slot, h], a_sem.at[slot, h])

    def own_copies(p, j):
        g, q = bufs[p].at[me, j], p % 2
        return [rcopy(g, g, isend.at[q, 0, j], irecv.at[q, 0, j], to_x),
                rcopy(g, g, isend.at[q, 1, j], irecv.at[q, 1, j], to_y),
                rcopy(g, g, dsend.at[q, 0, j], drecv.at[q, 0, j], partner)]

    def relay_x(p, j):
        g, q, half = bufs[p], p % 2, bufs[p].shape[2] // 2
        g = g.at[to_y, j, pl.ds(0, half)]
        return rcopy(g, g, isend.at[q, 2, j], irecv.at[q, 2, j], to_x)

    def relay_y(p, j):
        g, q, half = bufs[p], p % 2, bufs[p].shape[2] // 2
        g = g.at[to_x, j, pl.ds(half, half)]
        return rcopy(g, g, isend.at[q, 3, j], irecv.at[q, 3, j], to_y)

    def forward(p, m, j):
        g, q = bufs[p].at[chip_of(m) * 2 + core, j], p % 2
        return rcopy(g, g, dsend.at[q, m, j], drecv.at[q, m, j], partner)

    def arrive_xy(p, j):
        q = p % 2
        g = bufs[p].at[to_x, j]
        rcopy(g, g, isend.at[q, 0, j], irecv.at[q, 0, j], to_x).wait_recv()
        relay_y(p, j).start()
        forward(p, 1, j).start()
        g = bufs[p].at[to_y, j]
        rcopy(g, g, isend.at[q, 1, j], irecv.at[q, 1, j], to_y).wait_recv()
        relay_x(p, j).start()
        forward(p, 2, j).start()

    def arrive_d(p, j):
        q, half = p % 2, bufs[p].shape[2] // 2
        g = bufs[p].at[to_d, j, pl.ds(0, half)]
        rcopy(g, g, isend.at[q, 2, j], irecv.at[q, 2, j], to_x).wait_recv()
        g = bufs[p].at[to_d, j, pl.ds(half, half)]
        rcopy(g, g, isend.at[q, 3, j], irecv.at[q, 3, j], to_y).wait_recv()
        forward(p, 3, j).start()

    def arrive_core(p, m, j):
        q = p % 2
        g = bufs[p].at[chip_dyn(m) * 2 + 1 - core, j]
        rcopy(g, g, dsend.at[q, m, j], drecv.at[q, m, j], partner).wait_recv()

    def wait_sends(p, j):
        for copy in own_copies(p, j) + [relay_x(p, j), relay_y(p, j)] + [forward(p, m, j) for m in (1, 2, 3)]:
            copy.wait_send()

    peers = [chip_of(m) * 2 + lax.rem(core + c, 2) for m, c in ((3, 0), (3, 1), (1, 0), (1, 1), (2, 0), (2, 1), (0, 1))]

    def tile_copies(buf, send, recv):
        return [rcopy(buf.at[me], buf.at[me], send.at[k], recv.at[k], dev) for k, dev in enumerate(peers)]

    def slice_copies(src, dst, send, recv):
        return [rcopy(src.at[dev], dst.at[me], send.at[k], recv.at[k], dev) for k, dev in enumerate(peers)]

    def wait_tiles(copies, buf, send, recv):
        for k, dev in enumerate(peers):
            copies[k].wait_send()
            rcopy(buf.at[dev], buf.at[dev], send.at[k], recv.at[k], dev).wait_recv()

    sum_a = rcopy(s2.at[1 - core], ta, rsend.at[0], rrecv.at[0], partner)
    sum_b = [rcopy(hb.at[chip_of(m)], tb.at[m - 1], rsend.at[m], rrecv.at[m], chip_of(m) * 2 + core) for m in (1, 2, 3)]
    sum_c = [rcopy(s2.at[core, chip], s2.at[core, chip], rsend.at[3 + m], rrecv.at[3 + m], chip_of(m) * 2 + core)
             for m in (1, 2, 3)]
    sum_d = rcopy(s2.at[core], tc.at[core], rsend.at[7], rrecv.at[7], partner)

    def sum_two():
        sum_a.wait()
        hb[...] = s2[core] + ta[...]

    def sum_three():
        for copy in sum_b:
            copy.start()

    def sum_four():
        for copy in sum_b:
            copy.wait()
        s2[core, chip] = hb[chip] + tb[0] + tb[1] + tb[2]
        for copy in sum_c:
            copy.start()

    def sum_five():
        for m, copy in enumerate(sum_c, 1):
            copy.wait_send()
            g = s2.at[core, chip_of(m)]
            rcopy(g, g, rsend.at[3 + m], rrecv.at[3 + m], chip_of(m) * 2 + core).wait_recv()
        sum_d.start()
        tc[core] = s2[core]

    def sum_last():
        sum_d.wait_send()
        rcopy(tc.at[1 - core], tc.at[1 - core], rsend.at[7], rrecv.at[7], partner).wait_recv()

    barrier = pltpu.get_barrier_semaphore()
    for dev in peers:
        pl.semaphore_signal(barrier, inc=1, device_id=(dev,), device_id_type=MESH)
    x_copies = [pltpu.make_async_copy(x_hbm.at[j], xg.at[me, j], x_sem.at[j]) for j in range(CHUNKS)]
    small = [pltpu.make_async_copy(src, dst, w_sem.at[k]) for k, (src, dst) in enumerate(
        ((w1_hbm, w1_ref), (w2_hbm, w2_ref), (lab_hbm, lab_ref), (mask_hbm, mask_ref)))]
    for copy in x_copies + small:
        copy.start()
    for s in range(SLOTS):
        for copy in a_copies(jnp.int32(s), s):
            copy.start()
    cnt[me] = jnp.zeros(cnt.shape[1:], F32)
    los[me] = jnp.zeros(los.shape[1:], F32)
    pl.semaphore_wait(barrier, len(peers))
    for j, copy in enumerate(x_copies):
        copy.wait()
        for send in own_copies(0, j):
            send.start()

    for copy in small:
        copy.wait()
    w1t[...] = w1_ref[...].T.astype(BF16)
    cnt[me, 0:1, :] = jnp.sum(mask_ref[...].astype(F32), axis=0)

    def operands(p, m, j):
        refs = []
        for h in (0, 1):
            dev = chip_dyn(m) * 2 + h
            if p == 0:
                lhs[h, :hidden, :] = nt(w1t[...], xg[dev, j]).astype(BF16)
                refs.append(lhs.at[h, pl.ds(0, hidden)])
            elif p == 1:
                lhs[h] = nn(w2t[...], hg[dev, j]).astype(BF16)
                refs.append(lhs.at[h])
            else:
                refs.append(bufs[p].at[dev, j])
        return refs

    def product(refs, slot, rc):
        rows = pl.ds(rc * CHUNK, CHUNK) if isinstance(rc, int) else pl.ds(pl.multiple_of(rc * CHUNK, CHUNK), CHUNK)
        return nt(refs[0][...], ring[slot, 0, rows, :]) + nt(refs[1][...], ring[slot, 1, rows, :])

    def finish_one(rc):
        z = acc1[rc]
        hg[me, rc] = jnp.maximum(z, 0.0).astype(BF16)

    def finish_two(rc):
        for b in range(CHUNK // LANES):
            lanes = pl.ds(b * LANES, LANES)
            z = acc2[rc, :, lanes]
            index = lax.broadcasted_iota(jnp.int32, z.shape, 0)
            z = jnp.where(index < classes, z, -jnp.inf)
            top = jnp.max(z, axis=0, keepdims=True)
            e = jnp.exp(z - top)
            total = jnp.sum(e, axis=0, keepdims=True)
            hit = index == lab_ref[rc, :, lanes]
            picked = jnp.sum(jnp.where(hit, z, 0.0), axis=0, keepdims=True)
            mask_f = mask_ref[rc, :, lanes].astype(F32)
            los[me, 0:1, lanes] += mask_f * (jnp.log(total) + top - picked)
            onehot = jnp.where(hit, 1.0, 0.0)
            gg[me, rc, :, lanes] = ((e * (1.0 / total) - onehot) * (mask_f / mrow[:, lanes])).astype(BF16)

    def finish_three(rc):
        e2[rc, :rows_p, :] = acc2[rc].astype(BF16)
        dz = nn(w2b[...], e2[rc])
        dg[me, rc] = jnp.where(acc1[rc] > 0.0, dz, 0.0).astype(BF16)

    def finish_four(rc):
        return nt(xt[rc], acc1[rc].astype(BF16))

    def phase(p):
        acc = (acc1, acc2, acc2, acc1)[p]

        if p == 0:
            for copy in tile_copies(cnt, csend, crecv):
                copy.start()
            w2t[...] = jnp.zeros_like(w2t)
            w2t[:classes] = w2_ref[...].astype(BF16)
            wide = jnp.concatenate([w2t[...].astype(F32), jnp.zeros((w2b.shape[1] - rows_p, hidden), F32)], axis=0)
            w2b[...] = wide.T.astype(BF16)
            e2[:, rows_p:, :] = jnp.zeros((CHUNKS, e2.shape[1] - rows_p, CHUNK), BF16)
        if p == 1:
            wait_tiles(tile_copies(cnt, csend, crecv), cnt, csend, crecv)
            total = jnp.sum(jnp.sum(cnt[...], axis=0), axis=0, keepdims=True)
            mrow[...] = jnp.broadcast_to(jnp.sum(total, axis=1, keepdims=True), mrow.shape)
        if p == 2:
            for copy in tile_copies(los, lsend, lrecv):
                copy.start()
        if p == 3:
            grad = nt(e2[0], hg[me, 0])
            for rc in range(1, CHUNKS):
                grad = grad + nt(e2[rc], hg[me, rc])
            step2 = s2.shape[2]
            for k in range(8):
                s2[k // 4, k % 4] = grad[k * step2:(k + 1) * step2]
            sum_a.start()
            for rc in range(CHUNKS):
                xt[rc] = xg[me, rc].astype(F32).T.astype(BF16)
        acc[...] = jnp.zeros_like(acc)

        def step(i, carry):
            m, j = item(i)
            slot = lax.rem(i + p * ITEMS, SLOTS)

            if p > 0:
                @pl.when(i < 4)
                def _():
                    wait_sends(p - 1, i)

            arrive_core(p, m, j)
            for copy in a_copies(i, slot):
                copy.wait()
            refs = operands(p, m, j)
            acc[0] += product(refs, slot, 0)

            @pl.when((i >= 3) & (i < 11) & (lax.rem(i, 2) == 1))
            def _():
                arrive_xy(p, lax.div(i - 3, 2))

            @pl.when(i >= 11)
            def _():
                arrive_d(p, i - 11)

            if p == 3:
                pl.when(i == 4)(sum_two)
                pl.when(i == 10)(sum_three)

            for rc in range(1, CHUNKS):
                acc[rc] += product(refs, slot, rc)

            def prefetch():
                for copy in a_copies(lax.rem(i + SLOTS, ITEMS), slot):
                    copy.start()

            if p < 3:
                prefetch()
            else:
                pl.when(i + SLOTS < ITEMS)(prefetch)
            return carry

        lax.fori_loop(0, ITEMS - 1, step, 0)

        i = jnp.int32(ITEMS - 1)
        slot = (ITEMS - 1 + p * ITEMS) % SLOTS
        arrive_core(p, jnp.int32(3), CHUNKS - 1)
        for copy in a_copies(i, slot):
            copy.wait()
        refs = operands(p, jnp.int32(3), CHUNKS - 1)

        def finish(rc, carry):
            acc[rc] += product(refs, slot, rc)
            if p < 3:
                (finish_one, finish_two, finish_three)[p](rc)
                for copy in own_copies(p + 1, rc):
                    copy.start()
                return carry
            return carry + finish_four(rc)

        out = lax.fori_loop(0, CHUNKS, finish, jnp.zeros(dw1_ref.shape, F32) if p == 3 else 0)
        if p < 3:
            for copy in a_copies(jnp.int32((ITEMS - 1 + SLOTS) % ITEMS), slot):
                copy.start()
        return out

    for p in range(4):
        out = phase(p)

    step1, step2 = d1.shape[1], s2.shape[2]
    for k in range(8):
        d1[k] = out[k * step1:(k + 1) * step1]
    parts = slice_copies(d1, r1, p1send, p1recv)
    for copy in parts:
        copy.start()
    r1[me] = d1[me]
    sum_four()
    wait_tiles(tile_copies(los, lsend, lrecv), los, lsend, lrecv)
    total = jnp.sum(jnp.sum(los[...], axis=0), axis=0, keepdims=True)
    loss_ref[...] = jnp.sum(total, axis=1, keepdims=True) / mrow[:, 0:1]
    wait_tiles(parts, r1, p1send, p1recv)
    f1[me] = jnp.sum(r1[...], axis=0)
    whole = tile_copies(f1, f1send, f1recv)
    for copy in whole:
        copy.start()
    sum_five()
    for j in range(CHUNKS):
        wait_sends(3, j)
    sum_last()
    for k in range(8):
        n = min(step2, classes - k * step2)
        dw2_ref[k * step2:k * step2 + n, :] = tc[k // 4, k % 4, :n, :]
    wait_tiles(whole, f1, f1send, f1recv)
    for k in range(8):
        dw1_ref[k * step1:(k + 1) * step1, :] = f1[k]


def solution(mesh):
    axis = mesh.axis_names[0]

    def local_step(adj_rows, feat_rows, w_one, w_two, label_rows, mask_rows):
        f_in, hidden = w_one.shape
        classes = w_two.shape[1]
        rows_p = -(-classes // 32) * 32
        lanes_p = -(-classes // LANES) * LANES
        rows = adj_rows.shape[0]
        dma = pltpu.SemaphoreType.DMA
        vmem = pl.BlockSpec(memory_space=pltpu.VMEM)
        hbm = pl.BlockSpec(memory_space=pl.ANY)
        loss, dw1, dw2 = pl.pallas_call(
            functools.partial(gcn_kernel, axis, classes),
            name="gcn_step",
            out_shape=(jax.ShapeDtypeStruct((1, 1), F32), jax.ShapeDtypeStruct((f_in, hidden), F32),
                       jax.ShapeDtypeStruct((classes, hidden), F32)),
            in_specs=[hbm] * 6,
            out_specs=(vmem, vmem, vmem),
            scratch_shapes=[
                pltpu.VMEM((SLOTS, 2, rows, CHUNK), BF16),
                pltpu.VMEM((8, CHUNKS, CHUNK, f_in), BF16),
                pltpu.VMEM((8, CHUNKS, hidden, CHUNK), BF16),
                pltpu.VMEM((8, CHUNKS, rows_p, CHUNK), BF16),
                pltpu.VMEM((8, CHUNKS, hidden, CHUNK), BF16),
                pltpu.VMEM((CHUNKS, hidden, CHUNK), F32),
                pltpu.VMEM((CHUNKS, rows_p, CHUNK), F32),
                pltpu.VMEM((2, rows_p, CHUNK), BF16),
                pltpu.VMEM((CHUNKS, lanes_p, CHUNK), BF16),
                pltpu.VMEM((CHUNKS, f_in, CHUNK), BF16),
                pltpu.VMEM((f_in, hidden), F32),
                pltpu.VMEM((classes, hidden), F32),
                pltpu.VMEM((CHUNKS, 1, CHUNK), jnp.int32),
                pltpu.VMEM((CHUNKS, 1, CHUNK), jnp.int32),
                pltpu.VMEM((hidden, f_in), BF16),
                pltpu.VMEM((rows_p, hidden), BF16),
                pltpu.VMEM((hidden, lanes_p), BF16),
                pltpu.VMEM((8, 8, CHUNK), F32),
                pltpu.VMEM((8, 8, CHUNK), F32),
                pltpu.VMEM((1, CHUNK), F32),
                pltpu.VMEM((8, f_in // 8, hidden), F32),
                pltpu.VMEM((8, f_in // 8, hidden), F32),
                pltpu.VMEM((8, f_in // 8, hidden), F32),
                pltpu.VMEM((2, 4, lanes_p // 8, hidden), F32),
                pltpu.VMEM((4, lanes_p // 8, hidden), F32),
                pltpu.VMEM((2, 4, lanes_p // 8, hidden), F32),
                pltpu.VMEM((4, lanes_p // 8, hidden), F32),
                pltpu.VMEM((3, lanes_p // 8, hidden), F32),
                dma((SLOTS, 2)), dma((CHUNKS,)), dma((4,)),
                dma((2, 4, CHUNKS)), dma((2, 4, CHUNKS)), dma((2, 4, CHUNKS)), dma((2, 4, CHUNKS)),
                dma((7,)), dma((7,)), dma((7,)), dma((7,)), dma((7,)), dma((7,)), dma((7,)), dma((7,)),
                dma((8,)), dma((8,)),
            ],
            compiler_params=pltpu.CompilerParams(
                collective_id=0, has_side_effects=True, vmem_limit_bytes=67_000_000),
        )(adj_rows, feat_rows.reshape(CHUNKS, CHUNK, f_in), w_one, w_two.T,
          label_rows.reshape(CHUNKS, 1, CHUNK), mask_rows.reshape(CHUNKS, 1, CHUNK))
        return loss[0, 0], dw1, dw2.T

    return jax.shard_map(local_step, mesh=mesh, in_specs=(P(axis, None), P(axis, None), P(None, None), P(None, None), P(axis), P(axis)), out_specs=(P(), P(None, None), P(None, None)), check_vma=False)
```

```python
import functools

import jax
import jax.numpy as jnp
from jax import lax
from jax.experimental import pallas as pl
from jax.experimental.pallas import tpu as pltpu
from jax.sharding import PartitionSpec as P

MESH = pl.DeviceIdType.MESH
F32, BF16 = jnp.float32, jnp.bfloat16
SLOTS = 4
CHUNK = 512
CHUNKS = 4
ITEMS = 16
LANES = 128


def nt(left, right):
    return lax.dot_general(left, right, (((1,), (1,)), ((), ())), preferred_element_type=F32)


def nn(left, right):
    return jnp.dot(left, right, preferred_element_type=F32)


def gcn_kernel(axis, classes, a_hbm, x_hbm, w1_hbm, w2_hbm, lab_hbm, mask_hbm, loss_ref, dw1_ref, dw2_ref,
               ring, xg, hg, gg, dg, acc1, acc2, lhs, lhs2, e2, xt, w1_ref, w2_ref, lab_ref, mask_ref, w1t, w2t, w2b,
               cnt, los, mrow, d1, r1, f1, s2, ta, tc, hb, tb,
               a_sem, x_sem, w_sem, isend, irecv, dsend, drecv, csend, crecv, lsend, lrecv,
               p1send, p1recv, f1send, f1recv, rsend, rrecv):
    me = lax.axis_index(axis)
    core, chip = lax.rem(me, 2), lax.div(me, 2)
    cx, cy = lax.rem(chip, 2), lax.div(chip, 2)
    hidden = hg.shape[2]
    rows_p = gg.shape[2]

    def chip_of(m):
        return lax.rem(cy + m // 2, 2) * 2 + lax.rem(cx + m % 2, 2)

    def chip_dyn(m):
        return lax.rem(cy + lax.div(m, 2), 2) * 2 + lax.rem(cx + lax.rem(m, 2), 2)

    partner = chip * 2 + (1 - core)
    to_x, to_y, to_d = (chip_of(m) * 2 + core for m in (1, 2, 3))
    bufs = (xg, hg, gg, dg)

    def rcopy(src, dst, send, recv, dev):
        return pltpu.make_async_remote_copy(src_ref=src, dst_ref=dst, send_sem=send, recv_sem=recv,
                                            device_id=(dev,), device_id_type=MESH)

    def item(i):
        side = lax.div(lax.rem(i + 4, 16), 8)
        t = lax.rem(i + 12, 16)
        m = side * (1 + lax.rem(t, 2)) + 3 * lax.div(i, 12)
        j = side * lax.div(t, 2) + (1 - side) * lax.rem(i, 4)
        return m, j

    def a_copies(i, slot):
        m, j = item(i)
        first = chip_dyn(m) * (2 * CHUNK * CHUNKS) + j * CHUNK
        for h in (0, 1):
            cols = pl.ds(pl.multiple_of(first + h * CHUNK * CHUNKS, CHUNK), CHUNK)
            yield pltpu.make_async_copy(a_hbm.at[:, cols], ring.at[slot, h], a_sem.at[slot, h])

    def own_copies(p, j):
        g, q = bufs[p].at[me, j], p % 2
        return [rcopy(g, g, isend.at[q, 0, j], irecv.at[q, 0, j], to_x),
                rcopy(g, g, isend.at[q, 1, j], irecv.at[q, 1, j], to_y),
                rcopy(g, g, dsend.at[q, 0, j], drecv.at[q, 0, j], partner)]

    def relay_x(p, j):
        g, q, half = bufs[p], p % 2, bufs[p].shape[2] // 2
        g = g.at[to_y, j, pl.ds(0, half)]
        return rcopy(g, g, isend.at[q, 2, j], irecv.at[q, 2, j], to_x)

    def relay_y(p, j):
        g, q, half = bufs[p], p % 2, bufs[p].shape[2] // 2
        g = g.at[to_x, j, pl.ds(half, half)]
        return rcopy(g, g, isend.at[q, 3, j], irecv.at[q, 3, j], to_y)

    def forward(p, m, j):
        g, q = bufs[p].at[chip_of(m) * 2 + core, j], p % 2
        return rcopy(g, g, dsend.at[q, m, j], drecv.at[q, m, j], partner)

    def arrive_xy(p, j):
        q = p % 2
        g = bufs[p].at[to_x, j]
        rcopy(g, g, isend.at[q, 0, j], irecv.at[q, 0, j], to_x).wait_recv()
        relay_y(p, j).start()
        forward(p, 1, j).start()
        g = bufs[p].at[to_y, j]
        rcopy(g, g, isend.at[q, 1, j], irecv.at[q, 1, j], to_y).wait_recv()
        relay_x(p, j).start()
        forward(p, 2, j).start()

    def arrive_d(p, j):
        q, half = p % 2, bufs[p].shape[2] // 2
        g = bufs[p].at[to_d, j, pl.ds(0, half)]
        rcopy(g, g, isend.at[q, 2, j], irecv.at[q, 2, j], to_x).wait_recv()
        g = bufs[p].at[to_d, j, pl.ds(half, half)]
        rcopy(g, g, isend.at[q, 3, j], irecv.at[q, 3, j], to_y).wait_recv()
        forward(p, 3, j).start()

    def arrive_core(p, m, j):
        q = p % 2
        g = bufs[p].at[chip_dyn(m) * 2 + 1 - core, j]
        rcopy(g, g, dsend.at[q, m, j], drecv.at[q, m, j], partner).wait_recv()

    def wait_sends(p, j):
        for copy in own_copies(p, j) + [relay_x(p, j), relay_y(p, j)] + [forward(p, m, j) for m in (1, 2, 3)]:
            copy.wait_send()

    peers = [chip_of(m) * 2 + lax.rem(core + c, 2) for m, c in ((3, 0), (3, 1), (1, 0), (1, 1), (2, 0), (2, 1), (0, 1))]

    def tile_copies(buf, send, recv):
        return [rcopy(buf.at[me], buf.at[me], send.at[k], recv.at[k], dev) for k, dev in enumerate(peers)]

    def slice_copies(src, dst, send, recv):
        return [rcopy(src.at[dev], dst.at[me], send.at[k], recv.at[k], dev) for k, dev in enumerate(peers)]

    def wait_tiles(copies, buf, send, recv):
        for k, dev in enumerate(peers):
            copies[k].wait_send()
            rcopy(buf.at[dev], buf.at[dev], send.at[k], recv.at[k], dev).wait_recv()

    sum_a = rcopy(s2.at[1 - core], ta, rsend.at[0], rrecv.at[0], partner)
    sum_b = [rcopy(hb.at[chip_of(m)], tb.at[m - 1], rsend.at[m], rrecv.at[m], chip_of(m) * 2 + core) for m in (1, 2, 3)]
    sum_c = [rcopy(s2.at[core, chip], s2.at[core, chip], rsend.at[3 + m], rrecv.at[3 + m], chip_of(m) * 2 + core)
             for m in (1, 2, 3)]
    sum_d = rcopy(s2.at[core], tc.at[core], rsend.at[7], rrecv.at[7], partner)

    def sum_two():
        sum_a.wait()
        hb[...] = s2[core] + ta[...]

    def sum_three():
        for copy in sum_b:
            copy.start()

    def sum_four():
        for copy in sum_b:
            copy.wait()
        s2[core, chip] = hb[chip] + tb[0] + tb[1] + tb[2]
        for copy in sum_c:
            copy.start()

    def sum_five():
        for m, copy in enumerate(sum_c, 1):
            copy.wait_send()
            g = s2.at[core, chip_of(m)]
            rcopy(g, g, rsend.at[3 + m], rrecv.at[3 + m], chip_of(m) * 2 + core).wait_recv()
        sum_d.start()
        tc[core] = s2[core]

    def sum_last():
        sum_d.wait_send()
        rcopy(tc.at[1 - core], tc.at[1 - core], rsend.at[7], rrecv.at[7], partner).wait_recv()

    barrier = pltpu.get_barrier_semaphore()
    for dev in (to_x, to_y, partner):
        pl.semaphore_signal(barrier, inc=1, device_id=(dev,), device_id_type=MESH)
    x_copies = [pltpu.make_async_copy(x_hbm.at[j], xg.at[me, j], x_sem.at[j]) for j in range(CHUNKS)]
    small = [pltpu.make_async_copy(src, dst, w_sem.at[k]) for k, (src, dst) in enumerate(
        ((w1_hbm, w1_ref), (w2_hbm, w2_ref), (lab_hbm, lab_ref), (mask_hbm, mask_ref)))]
    for copy in x_copies + small:
        copy.start()
    for s in range(SLOTS):
        for copy in a_copies(jnp.int32(s), s):
            copy.start()
    cnt[me] = jnp.zeros(cnt.shape[1:], F32)
    los[me] = jnp.zeros(los.shape[1:], F32)
    pl.semaphore_wait(barrier, 3)
    for j, copy in enumerate(x_copies):
        copy.wait()
        for send in own_copies(0, j):
            send.start()

    for copy in small:
        copy.wait()
    w1t[...] = w1_ref[...].T.astype(BF16)
    cnt[me, 0:1, :] = jnp.sum(mask_ref[...].astype(F32), axis=0)

    def prepare(p, buf, m, j, h):
        dev = chip_dyn(m) * 2 + h
        if p == 0:
            buf[h, :hidden, :] = nt(w1t[...], xg[dev, j]).astype(BF16)
        else:
            buf[h] = nn(w2t[...], hg[dev, j]).astype(BF16)

    def operands(p, buf, m, j):
        if p == 0:
            return [buf.at[h, pl.ds(0, hidden)] for h in (0, 1)]
        if p == 1:
            return [buf.at[h] for h in (0, 1)]
        return [bufs[p].at[chip_dyn(m) * 2 + h, j] for h in (0, 1)]

    def product(refs, slot, rc):
        rows = pl.ds(rc * CHUNK, CHUNK) if isinstance(rc, int) else pl.ds(pl.multiple_of(rc * CHUNK, CHUNK), CHUNK)
        return nt(refs[0][...], ring[slot, 0, rows, :]) + nt(refs[1][...], ring[slot, 1, rows, :])

    def label_count():
        wait_tiles(tile_copies(cnt, csend, crecv), cnt, csend, crecv)
        total = jnp.sum(jnp.sum(cnt[...], axis=0), axis=0, keepdims=True)
        mrow[...] = jnp.broadcast_to(jnp.sum(total, axis=1, keepdims=True), mrow.shape)

    def finish_one(rc):
        z = acc1[rc]
        hg[me, rc] = jnp.maximum(z, 0.0).astype(BF16)

    def finish_two(rc):
        for b in range(CHUNK // LANES):
            lanes = pl.ds(b * LANES, LANES)
            z = acc2[rc, :, lanes]
            index = lax.broadcasted_iota(jnp.int32, z.shape, 0)
            z = jnp.where(index < classes, z, -jnp.inf)
            top = jnp.max(z, axis=0, keepdims=True)
            e = jnp.exp(z - top)
            total = jnp.sum(e, axis=0, keepdims=True)
            hit = index == lab_ref[rc, :, lanes]
            picked = jnp.sum(jnp.where(hit, z, 0.0), axis=0, keepdims=True)
            mask_f = mask_ref[rc, :, lanes].astype(F32)
            los[me, 0:1, lanes] += mask_f * (jnp.log(total) + top - picked)
            onehot = jnp.where(hit, 1.0, 0.0)
            gg[me, rc, :, lanes] = ((e * (1.0 / total) - onehot) * (mask_f / mrow[:, lanes])).astype(BF16)

    def finish_three(rc):
        e2[rc, :rows_p, :] = acc2[rc].astype(BF16)
        dz = nn(w2b[...], e2[rc])
        dg[me, rc] = jnp.where(acc1[rc] > 0.0, dz, 0.0).astype(BF16)

    def finish_four(rc):
        return nt(xt[rc], acc1[rc].astype(BF16))

    def phase(p):
        acc = (acc1, acc2, acc2, acc1)[p]

        if p == 0:
            w2t[...] = jnp.zeros_like(w2t)
            w2t[:classes] = w2_ref[...].astype(BF16)
            wide = jnp.concatenate([w2t[...].astype(F32), jnp.zeros((w2b.shape[1] - rows_p, hidden), F32)], axis=0)
            w2b[...] = wide.T.astype(BF16)
            e2[:, rows_p:, :] = jnp.zeros((CHUNKS, e2.shape[1] - rows_p, CHUNK), BF16)
        if p == 1:
            for copy in tile_copies(cnt, csend, crecv):
                copy.start()
        if p == 2:
            for copy in tile_copies(los, lsend, lrecv):
                copy.start()
        if p == 3:
            grad = nt(e2[0], hg[me, 0])
            for rc in range(1, CHUNKS):
                grad = grad + nt(e2[rc], hg[me, rc])
            step2 = s2.shape[2]
            for k in range(8):
                s2[k // 4, k % 4] = grad[k * step2:(k + 1) * step2]
            sum_a.start()
            for rc in range(CHUNKS):
                xt[rc] = xg[me, rc].astype(F32).T.astype(BF16)
        acc[...] = jnp.zeros_like(acc)

        def ready(i, slot):
            arrive_core(p, *item(i))
            for copy in a_copies(i, slot):
                copy.wait()

        def prefetch(i, slot):
            for copy in a_copies(lax.rem(i + SLOTS, ITEMS), slot):
                copy.start()

        def ahead(i, buf, other):
            slot = lax.rem(i, SLOTS)
            arrive_core(p, *item(i + 1))
            for copy in a_copies(i, slot):
                copy.wait()
            refs = operands(p, buf, *item(i))
            for h in (0, 1):
                prepare(p, other, *item(i + 1), h)
            for rc in range(CHUNKS):
                acc[rc] += product(refs, slot, rc)
            prefetch(i, slot)

        def pair(t, carry):
            @pl.when((t >= 1) & (t <= 4))
            def _():
                arrive_xy(p, t - 1)

            @pl.when(t >= 5)
            def _():
                arrive_d(p, 2 * t - 10)

            ahead(2 * t, lhs, lhs2)

            @pl.when(t >= 5)
            def _():
                arrive_d(p, 2 * t - 9)

            ahead(2 * t + 1, lhs2, lhs)
            return carry

        def step(i, carry):
            m, j = item(i)
            slot = lax.rem(i + p * ITEMS, SLOTS)

            if p > 0:
                @pl.when(i < 4)
                def _():
                    wait_sends(p - 1, i)

            ready(i, slot)
            if p == 1:
                for h in (0, 1):
                    prepare(p, lhs, m, j, h)
            refs = operands(p, lhs, m, j)
            acc[0] += product(refs, slot, 0)

            @pl.when((i >= 3) & (i < 11) & (lax.rem(i, 2) == 1))
            def _():
                arrive_xy(p, lax.div(i - 3, 2))

            @pl.when(i >= 11)
            def _():
                arrive_d(p, i - 11)

            if p == 1:
                pl.when(i == 8)(label_count)

            if p == 3:
                pl.when(i == 4)(sum_two)
                pl.when(i == 10)(sum_three)

            for rc in range(1, CHUNKS):
                acc[rc] += product(refs, slot, rc)

            if p < 3:
                prefetch(i, slot)
            else:
                pl.when(i + SLOTS < ITEMS)(lambda: prefetch(i, slot))
            return carry

        i = jnp.int32(ITEMS - 1)
        m, j = item(i)
        slot = (ITEMS - 1 + p * ITEMS) % SLOTS
        buf = lhs
        if p == 0:
            arrive_core(p, *item(jnp.int32(0)))
            for h in (0, 1):
                prepare(p, lhs, *item(jnp.int32(0)), h)
            lax.fori_loop(0, ITEMS // 2 - 1, pair, 0)
            ahead(jnp.int32(ITEMS - 2), lhs, lhs2)
            for copy in a_copies(i, slot):
                copy.wait()
            buf = lhs2
        else:
            lax.fori_loop(0, ITEMS - 1, step, 0)
            if p == 1:
                prepare(p, lhs, m, j, core)
            ready(i, slot)
            if p == 1:
                prepare(p, lhs, m, j, 1 - core)
        refs = operands(p, buf, m, j)

        def finish(rc, carry):
            acc[rc] += product(refs, slot, rc)
            if p < 3:
                (finish_one, finish_two, finish_three)[p](rc)
                for copy in own_copies(p + 1, rc):
                    copy.start()
                return carry
            return carry + finish_four(rc)

        out = lax.fori_loop(0, CHUNKS, finish, jnp.zeros(dw1_ref.shape, F32) if p == 3 else 0)
        if p < 3:
            prefetch(i, slot)
        return out

    for p in range(4):
        out = phase(p)

    step1, step2 = d1.shape[1], s2.shape[2]
    for k in range(8):
        d1[k] = out[k * step1:(k + 1) * step1]
    parts = slice_copies(d1, r1, p1send, p1recv)
    for copy in parts:
        copy.start()
    r1[me] = d1[me]
    sum_four()
    wait_tiles(tile_copies(los, lsend, lrecv), los, lsend, lrecv)
    total = jnp.sum(jnp.sum(los[...], axis=0), axis=0, keepdims=True)
    loss_ref[...] = jnp.sum(total, axis=1, keepdims=True) / mrow[:, 0:1]
    wait_tiles(parts, r1, p1send, p1recv)
    f1[me] = jnp.sum(r1[...], axis=0)
    whole = tile_copies(f1, f1send, f1recv)
    for copy in whole:
        copy.start()
    sum_five()
    for j in range(CHUNKS):
        wait_sends(3, j)
    sum_last()
    for k in range(8):
        n = min(step2, classes - k * step2)
        dw2_ref[k * step2:k * step2 + n, :] = tc[k // 4, k % 4, :n, :]
    wait_tiles(whole, f1, f1send, f1recv)
    for k in range(8):
        dw1_ref[k * step1:(k + 1) * step1, :] = f1[k]


def output_kernel(loss_in, dw1_in, dw2_in, loss_ref, dw1_ref, dw2_ref):
    loss_ref[...], dw1_ref[...], dw2_ref[...] = loss_in[...], dw1_in[...], dw2_in[...]


def solution(mesh):
    axis = mesh.axis_names[0]

    def local_step(adj_rows, feat_rows, w_one, w_two, label_rows, mask_rows):
        f_in, hidden = w_one.shape
        classes = w_two.shape[1]
        rows_p = -(-classes // 32) * 32
        lanes_p = -(-classes // LANES) * LANES
        rows = adj_rows.shape[0]
        dma = pltpu.SemaphoreType.DMA
        vmem = pl.BlockSpec(memory_space=pltpu.VMEM)
        hbm = pl.BlockSpec(memory_space=pl.ANY)
        loss, dw1, dw2 = pl.pallas_call(
            functools.partial(gcn_kernel, axis, classes),
            name="gcn_step",
            out_shape=(jax.ShapeDtypeStruct((1, 1), F32), jax.ShapeDtypeStruct((f_in, hidden), F32),
                       jax.ShapeDtypeStruct((classes, hidden), F32)),
            in_specs=[hbm] * 6,
            out_specs=(vmem, vmem, vmem),
            scratch_shapes=[
                pltpu.VMEM((SLOTS, 2, rows, CHUNK), BF16),
                pltpu.VMEM((8, CHUNKS, CHUNK, f_in), BF16),
                pltpu.VMEM((8, CHUNKS, hidden, CHUNK), BF16),
                pltpu.VMEM((8, CHUNKS, rows_p, CHUNK), BF16),
                pltpu.VMEM((8, CHUNKS, hidden, CHUNK), BF16),
                pltpu.VMEM((CHUNKS, hidden, CHUNK), F32),
                pltpu.VMEM((CHUNKS, rows_p, CHUNK), F32),
                pltpu.VMEM((2, rows_p, CHUNK), BF16),
                pltpu.VMEM((2, hidden, CHUNK), BF16),
                pltpu.VMEM((CHUNKS, lanes_p, CHUNK), BF16),
                pltpu.VMEM((CHUNKS, f_in, CHUNK), BF16),
                pltpu.VMEM((f_in, hidden), F32),
                pltpu.VMEM((classes, hidden), F32),
                pltpu.VMEM((CHUNKS, 1, CHUNK), jnp.int32),
                pltpu.VMEM((CHUNKS, 1, CHUNK), jnp.int32),
                pltpu.VMEM((hidden, f_in), BF16),
                pltpu.VMEM((rows_p, hidden), BF16),
                pltpu.VMEM((hidden, lanes_p), BF16),
                pltpu.VMEM((8, 8, CHUNK), F32),
                pltpu.VMEM((8, 8, CHUNK), F32),
                pltpu.VMEM((1, CHUNK), F32),
                pltpu.VMEM((8, f_in // 8, hidden), F32),
                pltpu.VMEM((8, f_in // 8, hidden), F32),
                pltpu.VMEM((8, f_in // 8, hidden), F32),
                pltpu.VMEM((2, 4, lanes_p // 8, hidden), F32),
                pltpu.VMEM((4, lanes_p // 8, hidden), F32),
                pltpu.VMEM((2, 4, lanes_p // 8, hidden), F32),
                pltpu.VMEM((4, lanes_p // 8, hidden), F32),
                pltpu.VMEM((3, lanes_p // 8, hidden), F32),
                dma((SLOTS, 2)), dma((CHUNKS,)), dma((4,)),
                dma((2, 4, CHUNKS)), dma((2, 4, CHUNKS)), dma((2, 4, CHUNKS)), dma((2, 4, CHUNKS)),
                dma((7,)), dma((7,)), dma((7,)), dma((7,)), dma((7,)), dma((7,)), dma((7,)), dma((7,)),
                dma((8,)), dma((8,)),
            ],
            compiler_params=pltpu.CompilerParams(
                collective_id=0, has_side_effects=True, vmem_limit_bytes=67_000_000),
        )(adj_rows, feat_rows.reshape(CHUNKS, CHUNK, f_in), w_one, w_two.T,
          label_rows.reshape(CHUNKS, 1, CHUNK), mask_rows.reshape(CHUNKS, 1, CHUNK))
        loss, dw1, dw2 = pl.pallas_call(
            output_kernel, name="outputs", in_specs=[vmem] * 3, out_specs=(vmem,) * 3,
            out_shape=tuple(jax.ShapeDtypeStruct(v.shape, v.dtype) for v in (loss, dw1, dw2)))(loss, dw1, dw2)
        return loss[0, 0], dw1, dw2.T

    return jax.shard_map(local_step, mesh=mesh, in_specs=(P(axis, None), P(axis, None), P(None, None), P(None, None), P(axis), P(axis)), out_specs=(P(), P(None, None), P(None, None)), check_vma=False)
```

```python
import functools

import jax
import jax.numpy as jnp
from jax import lax
from jax.experimental import pallas as pl
from jax.experimental.pallas import tpu as pltpu
from jax.sharding import PartitionSpec as P

MESH = pl.DeviceIdType.MESH
F32, BF16 = jnp.float32, jnp.bfloat16
SLOTS = 4
CHUNK = 512
CHUNKS = 4
ITEMS = 16
LANES = 128


def nt(left, right):
    return lax.dot_general(left, right, (((1,), (1,)), ((), ())), preferred_element_type=F32)


def nn(left, right):
    return jnp.dot(left, right, preferred_element_type=F32)


def gcn_kernel(axis, classes, a_hbm, x_hbm, w1_hbm, w2_hbm, lab_hbm, mask_hbm, loss_ref, dw1_ref, dw2_ref,
               ring, xg, hg, gg, dg, acc1, acc2, lhs, e2, xt, w1_ref, w2_ref, lab_ref, mask_ref, w1t, w2t, w2b,
               cnt, los, mrow, d1, r1, f1, s2, ta, tc, hb, tb,
               a_sem, x_sem, w_sem, isend, irecv, dsend, drecv, csend, crecv, lsend, lrecv,
               p1send, p1recv, f1send, f1recv, rsend, rrecv):
    me = lax.axis_index(axis)
    core, chip = lax.rem(me, 2), lax.div(me, 2)
    cx, cy = lax.rem(chip, 2), lax.div(chip, 2)
    hidden = hg.shape[2]
    rows_p = gg.shape[2]

    def chip_of(m):
        return lax.rem(cy + m // 2, 2) * 2 + lax.rem(cx + m % 2, 2)

    def chip_dyn(m):
        return lax.rem(cy + lax.div(m, 2), 2) * 2 + lax.rem(cx + lax.rem(m, 2), 2)

    partner = chip * 2 + (1 - core)
    to_x, to_y, to_d = (chip_of(m) * 2 + core for m in (1, 2, 3))
    bufs = (xg, hg, gg, dg)

    def rcopy(src, dst, send, recv, dev):
        return pltpu.make_async_remote_copy(src_ref=src, dst_ref=dst, send_sem=send, recv_sem=recv,
                                            device_id=(dev,), device_id_type=MESH)

    def item(i):
        side = lax.div(lax.rem(i + 4, 16), 8)
        t = lax.rem(i + 12, 16)
        m = side * (1 + lax.rem(t, 2)) + 3 * lax.div(i, 12)
        j = side * lax.div(t, 2) + (1 - side) * lax.rem(i, 4)
        return m, j

    def a_copies(i, slot):
        m, j = item(i)
        first = chip_dyn(m) * (2 * CHUNK * CHUNKS) + j * CHUNK
        for h in (0, 1):
            cols = pl.ds(pl.multiple_of(first + h * CHUNK * CHUNKS, CHUNK), CHUNK)
            yield pltpu.make_async_copy(a_hbm.at[:, cols], ring.at[slot, h], a_sem.at[slot, h])

    def own_copies(p, j):
        g, q = bufs[p].at[me, j], p % 2
        return [rcopy(g, g, isend.at[q, 0, j], irecv.at[q, 0, j], to_x),
                rcopy(g, g, isend.at[q, 1, j], irecv.at[q, 1, j], to_y),
                rcopy(g, g, dsend.at[q, 0, j], drecv.at[q, 0, j], partner)]

    def relay_x(p, j):
        g, q, half = bufs[p], p % 2, bufs[p].shape[2] // 2
        g = g.at[to_y, j, pl.ds(0, half)]
        return rcopy(g, g, isend.at[q, 2, j], irecv.at[q, 2, j], to_x)

    def relay_y(p, j):
        g, q, half = bufs[p], p % 2, bufs[p].shape[2] // 2
        g = g.at[to_x, j, pl.ds(half, half)]
        return rcopy(g, g, isend.at[q, 3, j], irecv.at[q, 3, j], to_y)

    def forward(p, m, j):
        g, q = bufs[p].at[chip_of(m) * 2 + core, j], p % 2
        return rcopy(g, g, dsend.at[q, m, j], drecv.at[q, m, j], partner)

    def arrive_xy(p, j):
        q = p % 2
        g = bufs[p].at[to_x, j]
        rcopy(g, g, isend.at[q, 0, j], irecv.at[q, 0, j], to_x).wait_recv()
        relay_y(p, j).start()
        forward(p, 1, j).start()
        g = bufs[p].at[to_y, j]
        rcopy(g, g, isend.at[q, 1, j], irecv.at[q, 1, j], to_y).wait_recv()
        relay_x(p, j).start()
        forward(p, 2, j).start()

    def arrive_d(p, j):
        q, half = p % 2, bufs[p].shape[2] // 2
        g = bufs[p].at[to_d, j, pl.ds(0, half)]
        rcopy(g, g, isend.at[q, 2, j], irecv.at[q, 2, j], to_x).wait_recv()
        g = bufs[p].at[to_d, j, pl.ds(half, half)]
        rcopy(g, g, isend.at[q, 3, j], irecv.at[q, 3, j], to_y).wait_recv()
        forward(p, 3, j).start()

    def arrive_core(p, m, j):
        q = p % 2
        g = bufs[p].at[chip_dyn(m) * 2 + 1 - core, j]
        rcopy(g, g, dsend.at[q, m, j], drecv.at[q, m, j], partner).wait_recv()

    def wait_sends(p, j):
        for copy in own_copies(p, j) + [relay_x(p, j), relay_y(p, j)] + [forward(p, m, j) for m in (1, 2, 3)]:
            copy.wait_send()

    peers = [chip_of(m) * 2 + lax.rem(core + c, 2) for m, c in ((3, 0), (3, 1), (1, 0), (1, 1), (2, 0), (2, 1), (0, 1))]

    def tile_copies(buf, send, recv):
        return [rcopy(buf.at[me], buf.at[me], send.at[k], recv.at[k], dev) for k, dev in enumerate(peers)]

    def slice_copies(src, dst, send, recv):
        return [rcopy(src.at[dev], dst.at[me], send.at[k], recv.at[k], dev) for k, dev in enumerate(peers)]

    def wait_tiles(copies, buf, send, recv):
        for k, dev in enumerate(peers):
            copies[k].wait_send()
            rcopy(buf.at[dev], buf.at[dev], send.at[k], recv.at[k], dev).wait_recv()

    sum_a = rcopy(s2.at[1 - core], ta, rsend.at[0], rrecv.at[0], partner)
    sum_b = [rcopy(hb.at[chip_of(m)], tb.at[m - 1], rsend.at[m], rrecv.at[m], chip_of(m) * 2 + core) for m in (1, 2, 3)]
    sum_c = [rcopy(s2.at[core, chip], s2.at[core, chip], rsend.at[3 + m], rrecv.at[3 + m], chip_of(m) * 2 + core)
             for m in (1, 2, 3)]
    sum_d = rcopy(s2.at[core], tc.at[core], rsend.at[7], rrecv.at[7], partner)

    def sum_two():
        sum_a.wait()
        hb[...] = s2[core] + ta[...]

    def sum_three():
        for copy in sum_b:
            copy.start()

    def sum_four():
        for copy in sum_b:
            copy.wait()
        s2[core, chip] = hb[chip] + tb[0] + tb[1] + tb[2]
        for copy in sum_c:
            copy.start()

    def sum_five():
        for m, copy in enumerate(sum_c, 1):
            copy.wait_send()
            g = s2.at[core, chip_of(m)]
            rcopy(g, g, rsend.at[3 + m], rrecv.at[3 + m], chip_of(m) * 2 + core).wait_recv()
        sum_d.start()
        tc[core] = s2[core]

    def sum_last():
        sum_d.wait_send()
        rcopy(tc.at[1 - core], tc.at[1 - core], rsend.at[7], rrecv.at[7], partner).wait_recv()

    barrier = pltpu.get_barrier_semaphore()
    for dev in (to_x, to_y, partner):
        pl.semaphore_signal(barrier, inc=1, device_id=(dev,), device_id_type=MESH)
    x_copies = [pltpu.make_async_copy(x_hbm.at[j], xg.at[me, j], x_sem.at[j]) for j in range(CHUNKS)]
    small = [pltpu.make_async_copy(src, dst, w_sem.at[k]) for k, (src, dst) in enumerate(
        ((w1_hbm, w1_ref), (w2_hbm, w2_ref), (lab_hbm, lab_ref), (mask_hbm, mask_ref)))]
    for copy in x_copies + small:
        copy.start()
    for s in range(SLOTS):
        for copy in a_copies(jnp.int32(s), s):
            copy.start()
    los[me] = jnp.zeros(los.shape[1:], F32)
    pl.semaphore_wait(barrier, 3)
    for j, copy in enumerate(x_copies):
        copy.wait()
        for send in own_copies(0, j):
            send.start()

    for copy in small:
        copy.wait()
    w1t[...] = w1_ref[...].T.astype(BF16)
    marks = jnp.sum(mask_ref[...].astype(F32), axis=0)
    cnt[me] = sum(marks[:, b * LANES:(b + 1) * LANES] for b in range(CHUNK // LANES))

    def place(i_parity, m, j, h):
        dev = chip_dyn(m) * 2 + h
        return (dg if i_parity == 0 else gg).at[dev, j, pl.ds(0, hidden)]

    def prepare_one(i_parity, m, j):
        for h in (0, 1):
            place(i_parity, m, j, h)[...] = nt(w1t[...], xg[chip_dyn(m) * 2 + h, j]).astype(BF16)

    def prepare_two(m, j, h):
        lhs[h] = nn(w2t[...], hg[chip_dyn(m) * 2 + h, j]).astype(BF16)

    def operands(p, i_parity, m, j):
        if p == 0:
            return [place(i_parity, m, j, h) for h in (0, 1)]
        if p == 1:
            return [lhs.at[h] for h in (0, 1)]
        return [bufs[p].at[chip_dyn(m) * 2 + h, j] for h in (0, 1)]

    def product(refs, slot, rc):
        rows = pl.ds(rc * CHUNK, CHUNK) if isinstance(rc, int) else pl.ds(pl.multiple_of(rc * CHUNK, CHUNK), CHUNK)
        return nt(refs[0][...], ring[slot, 0, rows, :]) + nt(refs[1][...], ring[slot, 1, rows, :])

    def label_count():
        wait_tiles(tile_copies(cnt, csend, crecv), cnt, csend, crecv)
        total = jnp.sum(cnt[...], axis=0)
        mrow[...] = jnp.broadcast_to(jnp.sum(total, axis=1, keepdims=True), mrow.shape)

    def finish_one(rc):
        z = acc1[rc]
        hg[me, rc] = jnp.maximum(z, 0.0).astype(BF16)

    def finish_two(rc):
        for b in range(CHUNK // LANES):
            lanes = pl.ds(b * LANES, LANES)
            z = acc2[rc, :, lanes]
            index = lax.broadcasted_iota(jnp.int32, z.shape, 0)
            z = jnp.where(index < classes, z, -jnp.inf)
            top = jnp.max(z, axis=0, keepdims=True)
            e = jnp.exp(z - top)
            total = jnp.sum(e, axis=0, keepdims=True)
            hit = index == lab_ref[rc, :, lanes]
            picked = jnp.sum(jnp.where(hit, z, 0.0), axis=0, keepdims=True)
            mask_f = mask_ref[rc, :, lanes].astype(F32)
            los[me] += mask_f * (jnp.log(total) + top - picked)
            onehot = jnp.where(hit, 1.0, 0.0)
            gg[me, rc, :, lanes] = ((e * (1.0 / total) - onehot) * (mask_f / mrow[:, lanes])).astype(BF16)

    def finish_three(rc):
        e2[rc, :rows_p, :] = acc2[rc].astype(BF16)
        dz = nn(w2b[...], e2[rc])
        dg[me, rc] = jnp.where(acc1[rc] > 0.0, dz, 0.0).astype(BF16)

    def finish_four(rc):
        return nt(xt[rc], acc1[rc].astype(BF16))

    def phase(p):
        acc = (acc1, acc2, acc2, acc1)[p]

        if p == 0:
            w2t[...] = jnp.zeros_like(w2t)
            w2t[:classes] = w2_ref[...].astype(BF16)
            wide = jnp.concatenate([w2t[...].astype(F32), jnp.zeros((w2b.shape[1] - rows_p, hidden), F32)], axis=0)
            w2b[...] = wide.T.astype(BF16)
            e2[:, rows_p:, :] = jnp.zeros((CHUNKS, e2.shape[1] - rows_p, CHUNK), BF16)
        if p == 1:
            for copy in tile_copies(cnt, csend, crecv):
                copy.start()
        if p == 2:
            for copy in tile_copies(los, lsend, lrecv):
                copy.start()
        if p == 3:
            grad = nt(e2[0], hg[me, 0])
            for rc in range(1, CHUNKS):
                grad = grad + nt(e2[rc], hg[me, rc])
            step2 = s2.shape[2]
            for k in range(8):
                s2[k // 4, k % 4] = grad[k * step2:(k + 1) * step2]
            sum_a.start()
            for rc in range(CHUNKS):
                xt[rc] = xg[me, rc].astype(F32).T.astype(BF16)
        acc[...] = jnp.zeros_like(acc)

        def ready(i, slot):
            arrive_core(p, *item(i))
            for copy in a_copies(i, slot):
                copy.wait()

        def prefetch(i, slot):
            for copy in a_copies(lax.rem(i + SLOTS, ITEMS), slot):
                copy.start()

        def ahead(i, parity):
            slot = lax.rem(i, SLOTS)
            arrive_core(p, *item(i + 1))
            for copy in a_copies(i, slot):
                copy.wait()
            refs = operands(p, parity, *item(i))
            prepare_one(1 - parity, *item(i + 1))
            for rc in range(CHUNKS):
                acc[rc] += product(refs, slot, rc)
            prefetch(i, slot)

        def pair(t, carry):
            @pl.when((t >= 1) & (t <= 4))
            def _():
                arrive_xy(p, t - 1)

            @pl.when(t == 5)
            def _():
                arrive_d(p, 0)

            ahead(2 * t, 0)

            @pl.when(t == 5)
            def _():
                arrive_d(p, 1)

            ahead(2 * t + 1, 1)
            return carry

        def step(i, carry):
            m, j = item(i)
            slot = lax.rem(i + p * ITEMS, SLOTS)

            if p > 0:
                @pl.when(i < 4)
                def _():
                    wait_sends(p - 1, i)

            ready(i, slot)
            if p == 1:
                for h in (0, 1):
                    prepare_two(m, j, h)
            refs = operands(p, 0, m, j)
            acc[0] += product(refs, slot, 0)

            @pl.when((i >= 3) & (i < 11) & (lax.rem(i, 2) == 1))
            def _():
                arrive_xy(p, lax.div(i - 3, 2))

            @pl.when(i >= 11)
            def _():
                arrive_d(p, i - 11)

            if p == 1:
                pl.when(i == 8)(label_count)

            if p == 3:
                pl.when(i == 4)(sum_two)
                pl.when(i == 10)(sum_three)

            for rc in range(1, CHUNKS):
                acc[rc] += product(refs, slot, rc)

            if p < 3:
                prefetch(i, slot)
            else:
                pl.when(i + SLOTS < ITEMS)(lambda: prefetch(i, slot))
            return carry

        tail = [jnp.int32(i) for i in (range(ITEMS - CHUNKS, ITEMS) if p == 0 else (ITEMS - 1,))]
        slots = [(int(i) + p * ITEMS) % SLOTS for i in (range(ITEMS - CHUNKS, ITEMS) if p == 0 else (ITEMS - 1,))]
        if p == 0:
            arrive_core(p, *item(jnp.int32(0)))
            prepare_one(0, *item(jnp.int32(0)))
            lax.fori_loop(0, (ITEMS - CHUNKS) // 2, pair, 0)
            arrive_d(p, 2)
            arrive_core(p, *item(tail[1]))
            prepare_one(1, *item(tail[1]))
            arrive_d(p, 3)
            for k in (2, 3):
                arrive_core(p, *item(tail[k]))
                prepare_one(k % 2, *item(tail[k]))
            for i, slot in zip(tail, slots):
                for copy in a_copies(i, slot):
                    copy.wait()
        else:
            lax.fori_loop(0, ITEMS - 1, step, 0)
            if p == 1:
                prepare_two(*item(tail[0]), core)
            ready(tail[0], slots[0])
            if p == 1:
                prepare_two(*item(tail[0]), 1 - core)

        def finish(rc, carry):
            for k, (i, slot) in enumerate(zip(tail, slots)):
                term = product(operands(p, k % 2, *item(i)), slot, rc)
                whole = term if k == 0 else whole + term
            acc[rc] += whole
            if p < 3:
                (finish_one, finish_two, finish_three)[p](rc)
                for copy in own_copies(p + 1, rc):
                    copy.start()
                return carry
            return carry + finish_four(rc)

        if p == 3:
            out = jnp.zeros(dw1_ref.shape, F32)
            for rc in range(CHUNKS):
                out = finish(rc, out)
            return out
        lax.fori_loop(0, CHUNKS, finish, 0)
        for i, slot in zip(tail, slots):
            prefetch(i, slot)

    for p in range(4):
        out = phase(p)

    step1, step2 = d1.shape[1], s2.shape[2]
    for k in range(8):
        d1[k] = out[k * step1:(k + 1) * step1]
    parts = slice_copies(d1, r1, p1send, p1recv)
    for copy in parts:
        copy.start()
    r1[me] = d1[me]
    sum_four()
    wait_tiles(tile_copies(los, lsend, lrecv), los, lsend, lrecv)
    total = jnp.sum(los[...], axis=0)
    loss_ref[...] = jnp.sum(total, axis=1, keepdims=True) / mrow[:, 0:1]
    wait_tiles(parts, r1, p1send, p1recv)
    f1[me] = jnp.sum(r1[...], axis=0)
    whole = tile_copies(f1, f1send, f1recv)
    for copy in whole:
        copy.start()
    sum_five()
    for j in range(CHUNKS):
        wait_sends(3, j)
    sum_last()
    for k in range(8):
        n = min(step2, classes - k * step2)
        dw2_ref[k * step2:k * step2 + n, :] = tc[k // 4, k % 4, :n, :]
    wait_tiles(whole, f1, f1send, f1recv)
    for k in range(8):
        dw1_ref[k * step1:(k + 1) * step1, :] = f1[k]


def output_kernel(loss_in, dw1_in, dw2_in, loss_ref, dw1_ref, dw2_ref):
    loss_ref[...], dw1_ref[...], dw2_ref[...] = loss_in[...], dw1_in[...], dw2_in[...]


def solution(mesh):
    axis = mesh.axis_names[0]

    def local_step(adj_rows, feat_rows, w_one, w_two, label_rows, mask_rows):
        f_in, hidden = w_one.shape
        classes = w_two.shape[1]
        rows_p = -(-classes // 32) * 32
        lanes_p = -(-classes // LANES) * LANES
        rows = adj_rows.shape[0]
        dma = pltpu.SemaphoreType.DMA
        vmem = pl.BlockSpec(memory_space=pltpu.VMEM)
        hbm = pl.BlockSpec(memory_space=pl.ANY)
        loss, dw1, dw2 = pl.pallas_call(
            functools.partial(gcn_kernel, axis, classes),
            name="gcn_step",
            out_shape=(jax.ShapeDtypeStruct((1, 1), F32), jax.ShapeDtypeStruct((f_in, hidden), F32),
                       jax.ShapeDtypeStruct((classes, hidden), F32)),
            in_specs=[hbm] * 6,
            out_specs=(vmem, vmem, vmem),
            scratch_shapes=[
                pltpu.VMEM((SLOTS, 2, rows, CHUNK), BF16),
                pltpu.VMEM((8, CHUNKS, CHUNK, f_in), BF16),
                pltpu.VMEM((8, CHUNKS, hidden, CHUNK), BF16),
                pltpu.VMEM((8, CHUNKS, rows_p, CHUNK), BF16),
                pltpu.VMEM((8, CHUNKS, hidden, CHUNK), BF16),
                pltpu.VMEM((CHUNKS, hidden, CHUNK), F32),
                pltpu.VMEM((CHUNKS, rows_p, CHUNK), F32),
                pltpu.VMEM((2, rows_p, CHUNK), BF16),
                pltpu.VMEM((CHUNKS, lanes_p, CHUNK), BF16),
                pltpu.VMEM((CHUNKS, f_in, CHUNK), BF16),
                pltpu.VMEM((f_in, hidden), F32),
                pltpu.VMEM((classes, hidden), F32),
                pltpu.VMEM((CHUNKS, 1, CHUNK), jnp.int32),
                pltpu.VMEM((CHUNKS, 1, CHUNK), jnp.int32),
                pltpu.VMEM((hidden, f_in), BF16),
                pltpu.VMEM((rows_p, hidden), BF16),
                pltpu.VMEM((hidden, lanes_p), BF16),
                pltpu.VMEM((8, 1, LANES), F32),
                pltpu.VMEM((8, 1, LANES), F32),
                pltpu.VMEM((1, CHUNK), F32),
                pltpu.VMEM((8, f_in // 8, hidden), F32),
                pltpu.VMEM((8, f_in // 8, hidden), F32),
                pltpu.VMEM((8, f_in // 8, hidden), F32),
                pltpu.VMEM((2, 4, lanes_p // 8, hidden), F32),
                pltpu.VMEM((4, lanes_p // 8, hidden), F32),
                pltpu.VMEM((2, 4, lanes_p // 8, hidden), F32),
                pltpu.VMEM((4, lanes_p // 8, hidden), F32),
                pltpu.VMEM((3, lanes_p // 8, hidden), F32),
                dma((SLOTS, 2)), dma((CHUNKS,)), dma((4,)),
                dma((2, 4, CHUNKS)), dma((2, 4, CHUNKS)), dma((2, 4, CHUNKS)), dma((2, 4, CHUNKS)),
                dma((7,)), dma((7,)), dma((7,)), dma((7,)), dma((7,)), dma((7,)), dma((7,)), dma((7,)),
                dma((8,)), dma((8,)),
            ],
            compiler_params=pltpu.CompilerParams(
                collective_id=0, has_side_effects=True, vmem_limit_bytes=67_000_000),
        )(adj_rows, feat_rows.reshape(CHUNKS, CHUNK, f_in), w_one, w_two.T,
          label_rows.reshape(CHUNKS, 1, CHUNK), mask_rows.reshape(CHUNKS, 1, CHUNK))
        loss, dw1, dw2 = pl.pallas_call(
            output_kernel, name="outputs", in_specs=[vmem] * 3, out_specs=(vmem,) * 3,
            out_shape=tuple(jax.ShapeDtypeStruct(v.shape, v.dtype) for v in (loss, dw1, dw2)))(loss, dw1, dw2)
        return loss[0, 0], dw1, dw2.T

    return jax.shard_map(local_step, mesh=mesh, in_specs=(P(axis, None), P(axis, None), P(None, None), P(None, None), P(axis), P(axis)), out_specs=(P(), P(None, None), P(None, None)), check_vma=False)
```

```python
import functools

import jax
import jax.numpy as jnp
from jax import lax
from jax.experimental import pallas as pl
from jax.experimental.pallas import tpu as pltpu
from jax.sharding import PartitionSpec as P

MESH = pl.DeviceIdType.MESH
F32, BF16 = jnp.float32, jnp.bfloat16
SLOTS = 5
CHUNK = 512
CHUNKS = 4
ITEMS = 16
LANES = 128


def nt(left, right):
    return lax.dot_general(left, right, (((1,), (1,)), ((), ())), preferred_element_type=F32)


def nn(left, right):
    return jnp.dot(left, right, preferred_element_type=F32)


def gcn_kernel(axis, classes, a_hbm, x_hbm, w1_hbm, w2_hbm, lab_hbm, mask_hbm, loss_ref, dw1_ref, dw2_ref,
               ring, xg, hg, gg, dg, acc1, acc2, lhs, e2, xt, w1_ref, w2_ref, lab_ref, mask_ref, w1t, w2t, w2b,
               cnt, los, mrow, d1, r1, f1, s2, ta, tc, hb, tb,
               a_sem, x_sem, w_sem, isend, irecv, dsend, drecv, csend, crecv, lsend, lrecv,
               p1send, p1recv, f1send, f1recv, rsend, rrecv):
    me = lax.axis_index(axis)
    core, chip = lax.rem(me, 2), lax.div(me, 2)
    cx, cy = lax.rem(chip, 2), lax.div(chip, 2)
    hidden = hg.shape[2]
    rows_p = gg.shape[2]

    def chip_of(m):
        return lax.rem(cy + m // 2, 2) * 2 + lax.rem(cx + m % 2, 2)

    def chip_dyn(m):
        return lax.rem(cy + lax.div(m, 2), 2) * 2 + lax.rem(cx + lax.rem(m, 2), 2)

    partner = chip * 2 + (1 - core)
    to_x, to_y, to_d = (chip_of(m) * 2 + core for m in (1, 2, 3))
    bufs = (xg, hg, gg, dg)

    def rcopy(src, dst, send, recv, dev):
        return pltpu.make_async_remote_copy(src_ref=src, dst_ref=dst, send_sem=send, recv_sem=recv,
                                            device_id=(dev,), device_id_type=MESH)

    def item(i):
        side = lax.div(lax.rem(i + 4, 16), 8)
        t = lax.rem(i + 12, 16)
        m = side * (1 + lax.rem(t, 2)) + 3 * lax.div(i, 12)
        j = side * lax.div(t, 2) + (1 - side) * lax.rem(i, 4)
        return m, j

    def a_copies(i, slot):
        m, j = item(i)
        first = chip_dyn(m) * (2 * CHUNK * CHUNKS) + j * CHUNK
        for h in (0, 1):
            cols = pl.ds(pl.multiple_of(first + h * CHUNK * CHUNKS, CHUNK), CHUNK)
            yield pltpu.make_async_copy(a_hbm.at[:, cols], ring.at[slot, h], a_sem.at[slot, h])

    def own_copies(p, j):
        g, q = bufs[p].at[me, j], p % 2
        return [rcopy(g, g, isend.at[q, 0, j], irecv.at[q, 0, j], to_x),
                rcopy(g, g, isend.at[q, 1, j], irecv.at[q, 1, j], to_y),
                rcopy(g, g, dsend.at[q, 0, j], drecv.at[q, 0, j], partner)]

    def relay_x(p, j):
        g, q, half = bufs[p], p % 2, bufs[p].shape[2] // 2
        g = g.at[to_y, j, pl.ds(0, half)]
        return rcopy(g, g, isend.at[q, 2, j], irecv.at[q, 2, j], to_x)

    def relay_y(p, j):
        g, q, half = bufs[p], p % 2, bufs[p].shape[2] // 2
        g = g.at[to_x, j, pl.ds(half, half)]
        return rcopy(g, g, isend.at[q, 3, j], irecv.at[q, 3, j], to_y)

    def forward(p, m, j):
        g, q = bufs[p].at[chip_of(m) * 2 + core, j], p % 2
        return rcopy(g, g, dsend.at[q, m, j], drecv.at[q, m, j], partner)

    def arrive_xy(p, j):
        q = p % 2
        g = bufs[p].at[to_x, j]
        rcopy(g, g, isend.at[q, 0, j], irecv.at[q, 0, j], to_x).wait_recv()
        relay_y(p, j).start()
        forward(p, 1, j).start()
        g = bufs[p].at[to_y, j]
        rcopy(g, g, isend.at[q, 1, j], irecv.at[q, 1, j], to_y).wait_recv()
        relay_x(p, j).start()
        forward(p, 2, j).start()

    def arrive_d(p, j):
        q, half = p % 2, bufs[p].shape[2] // 2
        g = bufs[p].at[to_d, j, pl.ds(0, half)]
        rcopy(g, g, isend.at[q, 2, j], irecv.at[q, 2, j], to_x).wait_recv()
        g = bufs[p].at[to_d, j, pl.ds(half, half)]
        rcopy(g, g, isend.at[q, 3, j], irecv.at[q, 3, j], to_y).wait_recv()
        forward(p, 3, j).start()

    def arrive_core(p, m, j):
        q = p % 2
        g = bufs[p].at[chip_dyn(m) * 2 + 1 - core, j]
        rcopy(g, g, dsend.at[q, m, j], drecv.at[q, m, j], partner).wait_recv()

    def wait_sends(p, j):
        for copy in own_copies(p, j) + [relay_x(p, j), relay_y(p, j)] + [forward(p, m, j) for m in (1, 2, 3)]:
            copy.wait_send()

    peers = [chip_of(m) * 2 + lax.rem(core + c, 2) for m, c in ((3, 0), (3, 1), (1, 0), (1, 1), (2, 0), (2, 1), (0, 1))]

    def tile_copies(buf, send, recv):
        return [rcopy(buf.at[me], buf.at[me], send.at[k], recv.at[k], dev) for k, dev in enumerate(peers)]

    def slice_copies(src, dst, send, recv):
        return [rcopy(src.at[dev], dst.at[me], send.at[k], recv.at[k], dev) for k, dev in enumerate(peers)]

    def wait_tiles(copies, buf, send, recv):
        for k, dev in enumerate(peers):
            copies[k].wait_send()
            rcopy(buf.at[dev], buf.at[dev], send.at[k], recv.at[k], dev).wait_recv()

    sum_a = rcopy(s2.at[1 - core], ta, rsend.at[0], rrecv.at[0], partner)
    sum_b = [rcopy(hb.at[chip_of(m)], tb.at[m - 1], rsend.at[m], rrecv.at[m], chip_of(m) * 2 + core) for m in (1, 2, 3)]
    sum_c = [rcopy(s2.at[core, chip], s2.at[core, chip], rsend.at[3 + m], rrecv.at[3 + m], chip_of(m) * 2 + core)
             for m in (1, 2, 3)]
    sum_d = rcopy(s2.at[core], tc.at[core], rsend.at[7], rrecv.at[7], partner)

    def sum_two():
        sum_a.wait()
        hb[...] = s2[core] + ta[...]

    def sum_three():
        for copy in sum_b:
            copy.start()

    def sum_four():
        for copy in sum_b:
            copy.wait()
        s2[core, chip] = hb[chip] + tb[0] + tb[1] + tb[2]
        for copy in sum_c:
            copy.start()

    def sum_five():
        for m, copy in enumerate(sum_c, 1):
            copy.wait_send()
            g = s2.at[core, chip_of(m)]
            rcopy(g, g, rsend.at[3 + m], rrecv.at[3 + m], chip_of(m) * 2 + core).wait_recv()
        sum_d.start()
        tc[core] = s2[core]

    def sum_last():
        sum_d.wait_send()
        rcopy(tc.at[1 - core], tc.at[1 - core], rsend.at[7], rrecv.at[7], partner).wait_recv()

    barrier = pltpu.get_barrier_semaphore()
    for dev in (to_x, to_y, partner):
        pl.semaphore_signal(barrier, inc=1, device_id=(dev,), device_id_type=MESH)
    x_copies = [pltpu.make_async_copy(x_hbm.at[j], xg.at[me, j], x_sem.at[j]) for j in range(CHUNKS)]
    small = [pltpu.make_async_copy(src, dst, w_sem.at[k]) for k, (src, dst) in enumerate(
        ((w1_hbm, w1_ref), (w2_hbm, w2_ref), (lab_hbm, lab_ref), (mask_hbm, mask_ref)))]
    for copy in x_copies + small:
        copy.start()
    for s in range(SLOTS):
        for copy in a_copies(jnp.int32(s), s):
            copy.start()
    los[me] = jnp.zeros(los.shape[1:], F32)
    pl.semaphore_wait(barrier, 3)
    for j, copy in enumerate(x_copies):
        copy.wait()
        for send in own_copies(0, j):
            send.start()

    for copy in small:
        copy.wait()
    w1t[...] = w1_ref[...].T.astype(BF16)
    marks = jnp.sum(mask_ref[...].astype(F32), axis=0)
    cnt[me] = sum(marks[:, b * LANES:(b + 1) * LANES] for b in range(CHUNK // LANES))

    def place(i_parity, m, j, h):
        dev = chip_dyn(m) * 2 + h
        return (dg if i_parity == 0 else gg).at[dev, j, pl.ds(0, hidden)]

    def prepare_one(i_parity, m, j):
        for h in (0, 1):
            place(i_parity, m, j, h)[...] = nt(w1t[...], xg[chip_dyn(m) * 2 + h, j]).astype(BF16)

    def prepare_two(m, j, h):
        lhs[h] = nn(w2t[...], hg[chip_dyn(m) * 2 + h, j]).astype(BF16)

    def operands(p, i_parity, m, j):
        if p == 0:
            return [place(i_parity, m, j, h) for h in (0, 1)]
        if p == 1:
            return [lhs.at[h] for h in (0, 1)]
        return [bufs[p].at[chip_dyn(m) * 2 + h, j] for h in (0, 1)]

    def product(refs, slot, rc):
        rows = pl.ds(rc * CHUNK, CHUNK) if isinstance(rc, int) else pl.ds(pl.multiple_of(rc * CHUNK, CHUNK), CHUNK)
        return nt(refs[0][...], ring[slot, 0, rows, :]) + nt(refs[1][...], ring[slot, 1, rows, :])

    def label_count():
        wait_tiles(tile_copies(cnt, csend, crecv), cnt, csend, crecv)
        total = jnp.sum(cnt[...], axis=0)
        mrow[...] = jnp.broadcast_to(jnp.sum(total, axis=1, keepdims=True), mrow.shape)

    def finish_one(rc):
        z = acc1[rc]
        hg[me, rc] = jnp.maximum(z, 0.0).astype(BF16)

    def finish_two(rc):
        for b in range(CHUNK // LANES):
            lanes = pl.ds(b * LANES, LANES)
            z = acc2[rc, :, lanes]
            index = lax.broadcasted_iota(jnp.int32, z.shape, 0)
            z = jnp.where(index < classes, z, -jnp.inf)
            top = jnp.max(z, axis=0, keepdims=True)
            e = jnp.exp(z - top)
            total = jnp.sum(e, axis=0, keepdims=True)
            hit = index == lab_ref[rc, :, lanes]
            picked = jnp.sum(jnp.where(hit, z, 0.0), axis=0, keepdims=True)
            mask_f = mask_ref[rc, :, lanes].astype(F32)
            los[me] += mask_f * (jnp.log(total) + top - picked)
            onehot = jnp.where(hit, 1.0, 0.0)
            gg[me, rc, :, lanes] = ((e * (1.0 / total) - onehot) * (mask_f / mrow[:, lanes])).astype(BF16)

    def finish_three(rc):
        e2[rc, :rows_p, :] = acc2[rc].astype(BF16)
        dz = nn(w2b[...], e2[rc])
        dg[me, rc] = jnp.where(acc1[rc] > 0.0, dz, 0.0).astype(BF16)

    def finish_four(rc):
        return nt(xt[rc], acc1[rc].astype(BF16))

    def phase(p):
        acc = (acc1, acc2, acc2, acc1)[p]

        if p == 0:
            w2t[...] = jnp.zeros_like(w2t)
            w2t[:classes] = w2_ref[...].astype(BF16)
            wide = jnp.concatenate([w2t[...].astype(F32), jnp.zeros((w2b.shape[1] - rows_p, hidden), F32)], axis=0)
            w2b[...] = wide.T.astype(BF16)
            e2[:, rows_p:, :] = jnp.zeros((CHUNKS, e2.shape[1] - rows_p, CHUNK), BF16)
        if p == 1:
            for copy in tile_copies(cnt, csend, crecv):
                copy.start()
        if p == 2:
            for copy in tile_copies(los, lsend, lrecv):
                copy.start()
        if p == 3:
            grad = nt(e2[0], hg[me, 0])
            for rc in range(1, CHUNKS):
                grad = grad + nt(e2[rc], hg[me, rc])
            step2 = s2.shape[2]
            for k in range(8):
                s2[k // 4, k % 4] = grad[k * step2:(k + 1) * step2]
            sum_a.start()
            for rc in range(CHUNKS):
                xt[rc] = xg[me, rc].astype(F32).T.astype(BF16)
        acc[...] = jnp.zeros_like(acc)

        def ready(i, slot):
            arrive_core(p, *item(i))
            for copy in a_copies(i, slot):
                copy.wait()

        def prefetch(i, slot):
            for copy in a_copies(lax.rem(i + SLOTS, ITEMS), slot):
                copy.start()

        def ahead(i, parity):
            slot = lax.rem(i, SLOTS)
            arrive_core(p, *item(i + 1))
            for copy in a_copies(i, slot):
                copy.wait()
            refs = operands(p, parity, *item(i))
            prepare_one(1 - parity, *item(i + 1))
            for rc in range(CHUNKS):
                acc[rc] += product(refs, slot, rc)
            prefetch(i, slot)

        def pair(t, carry):
            @pl.when((t >= 1) & (t <= 4))
            def _():
                arrive_xy(p, t - 1)

            @pl.when(t == 5)
            def _():
                arrive_d(p, 0)
                arrive_d(p, 1)

            ahead(2 * t, 0)

            @pl.when(t == 5)
            def _():
                arrive_d(p, 2)
                arrive_d(p, 3)

            ahead(2 * t + 1, 1)
            return carry

        def step(i, carry):
            m, j = item(i)
            slot = lax.rem(i + p * ITEMS, SLOTS)

            if p > 0:
                @pl.when(i < 4)
                def _():
                    wait_sends(p - 1, i)

            ready(i, slot)
            if p == 1:
                prepare_two(m, j, 1 - core)
            refs = operands(p, 0, m, j)
            if p != 1:
                acc[0] += product(refs, slot, 0)

            @pl.when((i >= 3) & (i < 11) & (lax.rem(i, 2) == 1))
            def _():
                arrive_xy(p, lax.div(i - 3, 2))

            @pl.when(i >= 11)
            def _():
                arrive_d(p, i - 11)

            if p == 1:
                pl.when(i == 8)(label_count)

            if p == 3:
                pl.when(i == 4)(sum_two)
                pl.when(i == 10)(sum_three)

            for rc in range(0 if p == 1 else 1, CHUNKS):
                acc[rc] += product(refs, slot, rc)
            if p == 1:
                prepare_two(*item(i + 1), core)

            if p < 3:
                prefetch(i, slot)
            else:
                pl.when(i + SLOTS < ITEMS)(lambda: prefetch(i, slot))
            return carry

        tail = [jnp.int32(i) for i in (range(ITEMS - CHUNKS, ITEMS) if p == 0 else (ITEMS - 1,))]
        slots = [(int(i) + p * ITEMS) % SLOTS for i in (range(ITEMS - CHUNKS, ITEMS) if p == 0 else (ITEMS - 1,))]
        if p == 0:
            arrive_core(p, *item(jnp.int32(0)))
            prepare_one(0, *item(jnp.int32(0)))
            lax.fori_loop(0, (ITEMS - CHUNKS) // 2, pair, 0)
            for k in (1, 2, 3):
                arrive_core(p, *item(tail[k]))
                prepare_one(k % 2, *item(tail[k]))
            for i, slot in zip(tail, slots):
                for copy in a_copies(i, slot):
                    copy.wait()
        else:
            if p == 1:
                prepare_two(*item(jnp.int32(0)), core)
            lax.fori_loop(0, ITEMS - 1, step, 0)
            ready(tail[0], slots[0])
            if p == 1:
                prepare_two(*item(tail[0]), 1 - core)

        def finish(rc, carry):
            for k, (i, slot) in enumerate(zip(tail, slots)):
                term = product(operands(p, k % 2, *item(i)), slot, rc)
                whole = term if k == 0 else whole + term
            acc[rc] += whole
            if p < 3:
                (finish_one, finish_two, finish_three)[p](rc)
                for copy in own_copies(p + 1, rc):
                    copy.start()
                return carry
            return carry + finish_four(rc)

        if p == 3:
            out = jnp.zeros(dw1_ref.shape, F32)
            for rc in range(CHUNKS):
                out = finish(rc, out)
            return out
        lax.fori_loop(0, CHUNKS, finish, 0)
        for i, slot in zip(tail, slots):
            prefetch(i, slot)

    for p in range(4):
        out = phase(p)

    step1, step2 = d1.shape[1], s2.shape[2]
    for k in range(8):
        d1[k] = out[k * step1:(k + 1) * step1]
    parts = slice_copies(d1, r1, p1send, p1recv)
    for copy in parts:
        copy.start()
    r1[me] = d1[me]
    sum_four()
    wait_tiles(tile_copies(los, lsend, lrecv), los, lsend, lrecv)
    total = jnp.sum(los[...], axis=0)
    loss_ref[...] = jnp.sum(total, axis=1, keepdims=True) / mrow[:, 0:1]
    wait_tiles(parts, r1, p1send, p1recv)
    f1[me] = jnp.sum(r1[...], axis=0)
    whole = tile_copies(f1, f1send, f1recv)
    for copy in whole:
        copy.start()
    sum_five()
    for j in range(CHUNKS):
        wait_sends(3, j)
    sum_last()
    for k in range(8):
        n = min(step2, classes - k * step2)
        dw2_ref[k * step2:k * step2 + n, :] = tc[k // 4, k % 4, :n, :]
    wait_tiles(whole, f1, f1send, f1recv)
    for k in range(8):
        dw1_ref[k * step1:(k + 1) * step1, :] = f1[k]


def output_kernel(loss_in, dw1_in, dw2_in, loss_ref, dw1_ref, dw2_ref):
    loss_ref[...], dw1_ref[...], dw2_ref[...] = loss_in[...], dw1_in[...], dw2_in[...]


def solution(mesh):
    axis = mesh.axis_names[0]

    def local_step(adj_rows, feat_rows, w_one, w_two, label_rows, mask_rows):
        f_in, hidden = w_one.shape
        classes = w_two.shape[1]
        rows_p = -(-classes // 32) * 32
        lanes_p = -(-classes // LANES) * LANES
        rows = adj_rows.shape[0]
        dma = pltpu.SemaphoreType.DMA
        vmem = pl.BlockSpec(memory_space=pltpu.VMEM)
        hbm = pl.BlockSpec(memory_space=pl.ANY)
        loss, dw1, dw2 = pl.pallas_call(
            functools.partial(gcn_kernel, axis, classes),
            name="gcn_step",
            out_shape=(jax.ShapeDtypeStruct((1, 1), F32), jax.ShapeDtypeStruct((f_in, hidden), F32),
                       jax.ShapeDtypeStruct((classes, hidden), F32)),
            in_specs=[hbm] * 6,
            out_specs=(vmem, vmem, vmem),
            scratch_shapes=[
                pltpu.VMEM((SLOTS, 2, rows, CHUNK), BF16),
                pltpu.VMEM((8, CHUNKS, CHUNK, f_in), BF16),
                pltpu.VMEM((8, CHUNKS, hidden, CHUNK), BF16),
                pltpu.VMEM((8, CHUNKS, rows_p, CHUNK), BF16),
                pltpu.VMEM((8, CHUNKS, hidden, CHUNK), BF16),
                pltpu.VMEM((CHUNKS, hidden, CHUNK), F32),
                pltpu.VMEM((CHUNKS, rows_p, CHUNK), F32),
                pltpu.VMEM((2, rows_p, CHUNK), BF16),
                pltpu.VMEM((CHUNKS, lanes_p, CHUNK), BF16),
                pltpu.VMEM((CHUNKS, f_in, CHUNK), BF16),
                pltpu.VMEM((f_in, hidden), F32),
                pltpu.VMEM((classes, hidden), F32),
                pltpu.VMEM((CHUNKS, 1, CHUNK), jnp.int32),
                pltpu.VMEM((CHUNKS, 1, CHUNK), jnp.int32),
                pltpu.VMEM((hidden, f_in), BF16),
                pltpu.VMEM((rows_p, hidden), BF16),
                pltpu.VMEM((hidden, lanes_p), BF16),
                pltpu.VMEM((8, 1, LANES), F32),
                pltpu.VMEM((8, 1, LANES), F32),
                pltpu.VMEM((1, CHUNK), F32),
                pltpu.VMEM((8, f_in // 8, hidden), F32),
                pltpu.VMEM((8, f_in // 8, hidden), F32),
                pltpu.VMEM((8, f_in // 8, hidden), F32),
                pltpu.VMEM((2, 4, lanes_p // 8, hidden), F32),
                pltpu.VMEM((4, lanes_p // 8, hidden), F32),
                pltpu.VMEM((2, 4, lanes_p // 8, hidden), F32),
                pltpu.VMEM((4, lanes_p // 8, hidden), F32),
                pltpu.VMEM((3, lanes_p // 8, hidden), F32),
                dma((SLOTS, 2)), dma((CHUNKS,)), dma((4,)),
                dma((2, 4, CHUNKS)), dma((2, 4, CHUNKS)), dma((2, 4, CHUNKS)), dma((2, 4, CHUNKS)),
                dma((7,)), dma((7,)), dma((7,)), dma((7,)), dma((7,)), dma((7,)), dma((7,)), dma((7,)),
                dma((8,)), dma((8,)),
            ],
            compiler_params=pltpu.CompilerParams(
                collective_id=0, has_side_effects=True, vmem_limit_bytes=67_000_000),
        )(adj_rows, feat_rows.reshape(CHUNKS, CHUNK, f_in), w_one, w_two.T,
          label_rows.reshape(CHUNKS, 1, CHUNK), mask_rows.reshape(CHUNKS, 1, CHUNK))
        loss, dw1, dw2 = pl.pallas_call(
            output_kernel, name="outputs", in_specs=[vmem] * 3, out_specs=(vmem,) * 3,
            out_shape=tuple(jax.ShapeDtypeStruct(v.shape, v.dtype) for v in (loss, dw1, dw2)))(loss, dw1, dw2)
        return loss[0, 0], dw1, dw2.T

    return jax.shard_map(local_step, mesh=mesh, in_specs=(P(axis, None), P(axis, None), P(None, None), P(None, None), P(axis), P(axis)), out_specs=(P(), P(None, None), P(None, None)), check_vma=False)
```

```python
import functools

import jax
import jax.numpy as jnp
from jax import lax
from jax.experimental import pallas as pl
from jax.experimental.pallas import tpu as pltpu
from jax.sharding import PartitionSpec as P

MESH = pl.DeviceIdType.MESH
F32, BF16 = jnp.float32, jnp.bfloat16
SLOTS = 5
CHUNK = 512
CHUNKS = 4
ITEMS = 16
LANES = 128


def nt(left, right):
    return lax.dot_general(left, right, (((1,), (1,)), ((), ())), preferred_element_type=F32)


def nn(left, right):
    return jnp.dot(left, right, preferred_element_type=F32)


def gcn_kernel(axis, classes, a_hbm, x_hbm, w1_hbm, w2_hbm, lab_hbm, mask_hbm, loss_ref, dw1_ref, dw2_ref,
               ring, xg, hg, gg, dg, acc1, acc2, lhs, e2, xt, w1_ref, w2_ref, lab_ref, mask_ref, w1t, w2t, w2b,
               cnt, los, mrow, d1, r1, f1, s2, ta, tc, hb, tb,
               a_sem, x_sem, w_sem, isend, irecv, dsend, drecv, csend, crecv, lsend, lrecv,
               p1send, p1recv, f1send, f1recv, rsend, rrecv):
    me = lax.axis_index(axis)
    core, chip = lax.rem(me, 2), lax.div(me, 2)
    cx, cy = lax.rem(chip, 2), lax.div(chip, 2)
    hidden = hg.shape[2]
    rows_p = gg.shape[2]

    def chip_of(m):
        return lax.rem(cy + m // 2, 2) * 2 + lax.rem(cx + m % 2, 2)

    def chip_dyn(m):
        return lax.rem(cy + lax.div(m, 2), 2) * 2 + lax.rem(cx + lax.rem(m, 2), 2)

    partner = chip * 2 + (1 - core)
    to_x, to_y, to_d = (chip_of(m) * 2 + core for m in (1, 2, 3))
    bufs = (xg, hg, gg, dg)

    def rcopy(src, dst, send, recv, dev):
        return pltpu.make_async_remote_copy(src_ref=src, dst_ref=dst, send_sem=send, recv_sem=recv,
                                            device_id=(dev,), device_id_type=MESH)

    def item(i):
        side = lax.div(lax.rem(i + 4, 16), 8)
        t = lax.rem(i + 12, 16)
        m = side * (1 + lax.rem(t, 2)) + 3 * lax.div(i, 12)
        j = side * lax.div(t, 2) + (1 - side) * lax.rem(i, 4)
        return m, j

    def a_copies(i, slot):
        m, j = item(i)
        first = chip_dyn(m) * (2 * CHUNK * CHUNKS) + j * CHUNK
        for h in (0, 1):
            cols = pl.ds(pl.multiple_of(first + h * CHUNK * CHUNKS, CHUNK), CHUNK)
            yield pltpu.make_async_copy(a_hbm.at[:, cols], ring.at[slot, h], a_sem.at[slot, h])

    def own_copies(p, j):
        g, q = bufs[p].at[me, j], p % 2
        return [rcopy(g, g, isend.at[q, 0, j], irecv.at[q, 0, j], to_x),
                rcopy(g, g, isend.at[q, 1, j], irecv.at[q, 1, j], to_y),
                rcopy(g, g, dsend.at[q, 0, j], drecv.at[q, 0, j], partner)]

    def relay_x(p, j):
        g, q, half = bufs[p], p % 2, bufs[p].shape[2] // 2
        g = g.at[to_y, j, pl.ds(0, half)]
        return rcopy(g, g, isend.at[q, 2, j], irecv.at[q, 2, j], to_x)

    def relay_y(p, j):
        g, q, half = bufs[p], p % 2, bufs[p].shape[2] // 2
        g = g.at[to_x, j, pl.ds(half, half)]
        return rcopy(g, g, isend.at[q, 3, j], irecv.at[q, 3, j], to_y)

    def forward(p, m, j):
        g, q = bufs[p].at[chip_of(m) * 2 + core, j], p % 2
        return rcopy(g, g, dsend.at[q, m, j], drecv.at[q, m, j], partner)

    def arrive_xy(p, j):
        q = p % 2
        g = bufs[p].at[to_x, j]
        rcopy(g, g, isend.at[q, 0, j], irecv.at[q, 0, j], to_x).wait_recv()
        relay_y(p, j).start()
        forward(p, 1, j).start()
        g = bufs[p].at[to_y, j]
        rcopy(g, g, isend.at[q, 1, j], irecv.at[q, 1, j], to_y).wait_recv()
        relay_x(p, j).start()
        forward(p, 2, j).start()

    def arrive_d(p, j):
        q, half = p % 2, bufs[p].shape[2] // 2
        g = bufs[p].at[to_d, j, pl.ds(0, half)]
        rcopy(g, g, isend.at[q, 2, j], irecv.at[q, 2, j], to_x).wait_recv()
        g = bufs[p].at[to_d, j, pl.ds(half, half)]
        rcopy(g, g, isend.at[q, 3, j], irecv.at[q, 3, j], to_y).wait_recv()
        forward(p, 3, j).start()

    def arrive_core(p, m, j):
        q = p % 2
        g = bufs[p].at[chip_dyn(m) * 2 + 1 - core, j]
        rcopy(g, g, dsend.at[q, m, j], drecv.at[q, m, j], partner).wait_recv()

    def wait_sends(p, j):
        for copy in own_copies(p, j) + [relay_x(p, j), relay_y(p, j)] + [forward(p, m, j) for m in (1, 2, 3)]:
            copy.wait_send()

    peers = [chip_of(m) * 2 + lax.rem(core + c, 2) for m, c in ((3, 0), (3, 1), (1, 0), (1, 1), (2, 0), (2, 1), (0, 1))]

    def tile_copies(buf, send, recv):
        return [rcopy(buf.at[me], buf.at[me], send.at[k], recv.at[k], dev) for k, dev in enumerate(peers)]

    def slice_copies(src, dst, send, recv):
        return [rcopy(src.at[dev], dst.at[me], send.at[k], recv.at[k], dev) for k, dev in enumerate(peers)]

    def wait_tiles(copies, buf, send, recv):
        for k, dev in enumerate(peers):
            copies[k].wait_send()
            rcopy(buf.at[dev], buf.at[dev], send.at[k], recv.at[k], dev).wait_recv()

    sum_a = rcopy(s2.at[1 - core], ta, rsend.at[0], rrecv.at[0], partner)
    sum_b = [rcopy(hb.at[chip_of(m)], tb.at[m - 1], rsend.at[m], rrecv.at[m], chip_of(m) * 2 + core) for m in (1, 2, 3)]
    sum_c = [rcopy(s2.at[core, chip], s2.at[core, chip], rsend.at[3 + m], rrecv.at[3 + m], chip_of(m) * 2 + core)
             for m in (1, 2, 3)]
    sum_d = rcopy(s2.at[core], tc.at[core], rsend.at[7], rrecv.at[7], partner)

    def sum_two():
        sum_a.wait()
        hb[...] = s2[core] + ta[...]

    def sum_three():
        for copy in sum_b:
            copy.start()

    def sum_four():
        for copy in sum_b:
            copy.wait()
        s2[core, chip] = hb[chip] + tb[0] + tb[1] + tb[2]
        for copy in sum_c:
            copy.start()

    def sum_five():
        for m, copy in enumerate(sum_c, 1):
            copy.wait_send()
            g = s2.at[core, chip_of(m)]
            rcopy(g, g, rsend.at[3 + m], rrecv.at[3 + m], chip_of(m) * 2 + core).wait_recv()
        sum_d.start()
        tc[core] = s2[core]

    def sum_last():
        sum_d.wait_send()
        rcopy(tc.at[1 - core], tc.at[1 - core], rsend.at[7], rrecv.at[7], partner).wait_recv()

    barrier = pltpu.get_barrier_semaphore()
    for dev in (to_x, to_y, partner):
        pl.semaphore_signal(barrier, inc=1, device_id=(dev,), device_id_type=MESH)
    x_copies = [pltpu.make_async_copy(x_hbm.at[j], xg.at[me, j], x_sem.at[j]) for j in range(CHUNKS)]
    small = [pltpu.make_async_copy(src, dst, w_sem.at[k]) for k, (src, dst) in enumerate(
        ((w1_hbm, w1_ref), (w2_hbm, w2_ref), (lab_hbm, lab_ref), (mask_hbm, mask_ref)))]
    for copy in x_copies + small:
        copy.start()
    for s in range(SLOTS):
        for copy in a_copies(jnp.int32(s), s):
            copy.start()
    los[me] = jnp.zeros(los.shape[1:], F32)
    pl.semaphore_wait(barrier, 3)
    for j, copy in enumerate(x_copies):
        copy.wait()
        for send in own_copies(0, j):
            send.start()

    for copy in small:
        copy.wait()
    w1t[...] = w1_ref[...].T.astype(BF16)
    marks = jnp.sum(mask_ref[...].astype(F32), axis=0)
    cnt[me] = sum(marks[:, b * LANES:(b + 1) * LANES] for b in range(CHUNK // LANES))

    def place(i_parity, m, j, h):
        dev = chip_dyn(m) * 2 + h
        return (dg if i_parity == 0 else gg).at[dev, j, pl.ds(0, hidden)]

    def prepare_one(i_parity, m, j):
        for h in (0, 1):
            place(i_parity, m, j, h)[...] = nt(w1t[...], xg[chip_dyn(m) * 2 + h, j]).astype(BF16)

    def prepare_two(m, j, h):
        lhs[h] = nn(w2t[...], hg[chip_dyn(m) * 2 + h, j]).astype(BF16)

    def operands(p, i_parity, m, j):
        if p == 0:
            return [place(i_parity, m, j, h) for h in (0, 1)]
        if p == 1:
            return [lhs.at[h] for h in (0, 1)]
        return [bufs[p].at[chip_dyn(m) * 2 + h, j] for h in (0, 1)]

    def product(refs, slot, rc):
        rows = pl.ds(rc * CHUNK, CHUNK) if isinstance(rc, int) else pl.ds(pl.multiple_of(rc * CHUNK, CHUNK), CHUNK)
        return nt(refs[0][...], ring[slot, 0, rows, :]) + nt(refs[1][...], ring[slot, 1, rows, :])

    def label_count():
        wait_tiles(tile_copies(cnt, csend, crecv), cnt, csend, crecv)
        total = jnp.sum(cnt[...], axis=0)
        mrow[...] = jnp.broadcast_to(jnp.sum(total, axis=1, keepdims=True), mrow.shape)

    def finish_one(rc):
        z = acc1[rc]
        hg[me, rc] = jnp.maximum(z, 0.0).astype(BF16)

    def finish_two(rc):
        for b in range(CHUNK // LANES):
            lanes = pl.ds(b * LANES, LANES)
            z = acc2[rc, :, lanes]
            index = lax.broadcasted_iota(jnp.int32, z.shape, 0)
            z = jnp.where(index < classes, z, -jnp.inf)
            top = jnp.max(z, axis=0, keepdims=True)
            e = jnp.exp(z - top)
            total = jnp.sum(e, axis=0, keepdims=True)
            hit = index == lab_ref[rc, :, lanes]
            picked = jnp.sum(jnp.where(hit, z, 0.0), axis=0, keepdims=True)
            mask_f = mask_ref[rc, :, lanes].astype(F32)
            los[me] += mask_f * (jnp.log(total) + top - picked)
            onehot = jnp.where(hit, 1.0, 0.0)
            gg[me, rc, :, lanes] = ((e * (1.0 / total) - onehot) * (mask_f / mrow[:, lanes])).astype(BF16)

    def finish_three(rc):
        e2[rc, :rows_p, :] = acc2[rc].astype(BF16)
        dz = nn(w2b[...], e2[rc])
        dg[me, rc] = jnp.where(acc1[rc] > 0.0, dz, 0.0).astype(BF16)

    def finish_four(rc, z):
        return nt(xt[rc], z.astype(BF16))

    def phase(p):
        acc = (acc1, acc2, acc2, acc1)[p]

        if p == 0:
            w2t[...] = jnp.zeros_like(w2t)
            w2t[:classes] = w2_ref[...].astype(BF16)
            wide = jnp.concatenate([w2t[...].astype(F32), jnp.zeros((w2b.shape[1] - rows_p, hidden), F32)], axis=0)
            w2b[...] = wide.T.astype(BF16)
            e2[:, rows_p:, :] = jnp.zeros((CHUNKS, e2.shape[1] - rows_p, CHUNK), BF16)
        if p == 1:
            for copy in tile_copies(cnt, csend, crecv):
                copy.start()
        if p == 2:
            for copy in tile_copies(los, lsend, lrecv):
                copy.start()
        if p == 3:
            grad = nt(e2[0], hg[me, 0])
            for rc in range(1, CHUNKS):
                grad = grad + nt(e2[rc], hg[me, rc])
            step2 = s2.shape[2]
            for k in range(8):
                s2[k // 4, k % 4] = grad[k * step2:(k + 1) * step2]
            sum_a.start()
            for rc in range(CHUNKS):
                xt[rc] = xg[me, rc].astype(F32).T.astype(BF16)
        acc[...] = jnp.zeros_like(acc)

        def ready(i, slot):
            arrive_core(p, *item(i))
            for copy in a_copies(i, slot):
                copy.wait()

        def prefetch(i, slot):
            for copy in a_copies(lax.rem(i + SLOTS, ITEMS), slot):
                copy.start()

        def ahead(i, parity):
            slot = lax.rem(i, SLOTS)
            arrive_core(p, *item(i + 1))
            for copy in a_copies(i, slot):
                copy.wait()
            refs = operands(p, parity, *item(i))
            prepare_one(1 - parity, *item(i + 1))
            for rc in range(CHUNKS):
                acc[rc] += product(refs, slot, rc)
            prefetch(i, slot)

        def pair(t, carry):
            @pl.when((t >= 1) & (t <= 4))
            def _():
                arrive_xy(p, t - 1)

            @pl.when(t == 5)
            def _():
                arrive_d(p, 0)
                arrive_d(p, 1)

            ahead(2 * t, 0)

            @pl.when(t == 5)
            def _():
                arrive_d(p, 2)
                arrive_d(p, 3)

            ahead(2 * t + 1, 1)
            return carry

        def step(i, carry):
            m, j = item(i)
            slot = lax.rem(i + p * ITEMS, SLOTS)

            if p > 0:
                @pl.when(i < 4)
                def _():
                    wait_sends(p - 1, i)

            ready(i, slot)
            if p == 1:
                prepare_two(m, j, 1 - core)
            refs = operands(p, 0, m, j)
            if p != 1:
                acc[0] += product(refs, slot, 0)

            @pl.when((i >= 3) & (i < 11) & (lax.rem(i, 2) == 1))
            def _():
                arrive_xy(p, lax.div(i - 3, 2))

            @pl.when((i >= 11) & (i < (ITEMS - 2 if p == 3 else ITEMS)))
            def _():
                arrive_d(p, i - 11)

            if p == 1:
                pl.when(i == 8)(label_count)

            if p == 3:
                pl.when(i == 4)(sum_two)
                pl.when(i == 10)(sum_three)

            for rc in range(0 if p == 1 else 1, CHUNKS):
                acc[rc] += product(refs, slot, rc)
            if p == 1:
                prepare_two(*item(i + 1), core)

            if p < 3:
                prefetch(i, slot)
            else:
                pl.when(i + SLOTS < ITEMS)(lambda: prefetch(i, slot))
            return carry

        tail = [jnp.int32(i) for i in (range(ITEMS - CHUNKS, ITEMS) if p == 0 else (ITEMS - 1,))]
        slots = [(int(i) + p * ITEMS) % SLOTS for i in (range(ITEMS - CHUNKS, ITEMS) if p == 0 else (ITEMS - 1,))]
        def half_operand(h):
            m, j = item(tail[0])
            return dg.at[chip_dyn(m) * 2 + h, j]

        if p == 0:
            arrive_core(p, *item(jnp.int32(0)))
            prepare_one(0, *item(jnp.int32(0)))
            lax.fori_loop(0, (ITEMS - CHUNKS) // 2, pair, 0)
            for k in (1, 2, 3):
                arrive_core(p, *item(tail[k]))
                prepare_one(k % 2, *item(tail[k]))
            for i, slot in zip(tail, slots):
                for copy in a_copies(i, slot):
                    copy.wait()
        else:
            if p == 1:
                prepare_two(*item(jnp.int32(0)), core)
            lax.fori_loop(0, ITEMS - 1, step, 0)
            if p == 3:
                arrive_d(p, CHUNKS - 1)
                for copy in a_copies(tail[0], slots[0]):
                    copy.wait()
                own = half_operand(core)
                for rc in range(CHUNKS):
                    acc[rc] += nt(own[...], ring[slots[0], core, pl.ds(rc * CHUNK, CHUNK), :])
                arrive_core(p, *item(tail[0]))
            else:
                ready(tail[0], slots[0])
            if p == 1:
                prepare_two(*item(tail[0]), 1 - core)

        def finish(rc, carry):
            if p == 3:
                rest = ring[slots[0], 1 - core, pl.ds(rc * CHUNK, CHUNK), :]
                return carry + finish_four(rc, acc[rc] + nt(half_operand(1 - core)[...], rest))
            for k, (i, slot) in enumerate(zip(tail, slots)):
                term = product(operands(p, k % 2, *item(i)), slot, rc)
                whole = term if k == 0 else whole + term
            acc[rc] += whole
            (finish_one, finish_two, finish_three)[p](rc)
            for copy in own_copies(p + 1, rc):
                copy.start()
            return carry

        if p == 3:
            out = jnp.zeros(dw1_ref.shape, F32)
            for rc in range(CHUNKS):
                out = finish(rc, out)
            return out
        lax.fori_loop(0, CHUNKS, finish, 0)
        for i, slot in zip(tail, slots):
            prefetch(i, slot)

    for p in range(4):
        out = phase(p)

    step1, step2 = d1.shape[1], s2.shape[2]
    for k in range(8):
        d1[k] = out[k * step1:(k + 1) * step1]
    parts = slice_copies(d1, r1, p1send, p1recv)
    for copy in parts:
        copy.start()
    r1[me] = d1[me]
    sum_four()
    wait_tiles(tile_copies(los, lsend, lrecv), los, lsend, lrecv)
    total = jnp.sum(los[...], axis=0)
    loss_ref[...] = jnp.sum(total, axis=1, keepdims=True) / mrow[:, 0:1]
    wait_tiles(parts, r1, p1send, p1recv)
    f1[me] = jnp.sum(r1[...], axis=0)
    whole = tile_copies(f1, f1send, f1recv)
    for copy in whole:
        copy.start()
    sum_five()
    for j in range(CHUNKS):
        wait_sends(3, j)
    sum_last()
    for k in range(8):
        n = min(step2, classes - k * step2)
        dw2_ref[k * step2:k * step2 + n, :] = tc[k // 4, k % 4, :n, :]
    wait_tiles(whole, f1, f1send, f1recv)
    for k in range(8):
        dw1_ref[k * step1:(k + 1) * step1, :] = f1[k]


def output_kernel(loss_in, dw1_in, dw2_in, loss_ref, dw1_ref, dw2_ref):
    loss_ref[...], dw1_ref[...], dw2_ref[...] = loss_in[...], dw1_in[...], dw2_in[...]


def solution(mesh):
    axis = mesh.axis_names[0]

    def local_step(adj_rows, feat_rows, w_one, w_two, label_rows, mask_rows):
        f_in, hidden = w_one.shape
        classes = w_two.shape[1]
        rows_p = -(-classes // 32) * 32
        lanes_p = -(-classes // LANES) * LANES
        rows = adj_rows.shape[0]
        dma = pltpu.SemaphoreType.DMA
        vmem = pl.BlockSpec(memory_space=pltpu.VMEM)
        hbm = pl.BlockSpec(memory_space=pl.ANY)
        loss, dw1, dw2 = pl.pallas_call(
            functools.partial(gcn_kernel, axis, classes),
            name="gcn_step",
            out_shape=(jax.ShapeDtypeStruct((1, 1), F32), jax.ShapeDtypeStruct((f_in, hidden), F32),
                       jax.ShapeDtypeStruct((classes, hidden), F32)),
            in_specs=[hbm] * 6,
            out_specs=(vmem, vmem, vmem),
            scratch_shapes=[
                pltpu.VMEM((SLOTS, 2, rows, CHUNK), BF16),
                pltpu.VMEM((8, CHUNKS, CHUNK, f_in), BF16),
                pltpu.VMEM((8, CHUNKS, hidden, CHUNK), BF16),
                pltpu.VMEM((8, CHUNKS, rows_p, CHUNK), BF16),
                pltpu.VMEM((8, CHUNKS, hidden, CHUNK), BF16),
                pltpu.VMEM((CHUNKS, hidden, CHUNK), F32),
                pltpu.VMEM((CHUNKS, rows_p, CHUNK), F32),
                pltpu.VMEM((2, rows_p, CHUNK), BF16),
                pltpu.VMEM((CHUNKS, lanes_p, CHUNK), BF16),
                pltpu.VMEM((CHUNKS, f_in, CHUNK), BF16),
                pltpu.VMEM((f_in, hidden), F32),
                pltpu.VMEM((classes, hidden), F32),
                pltpu.VMEM((CHUNKS, 1, CHUNK), jnp.int32),
                pltpu.VMEM((CHUNKS, 1, CHUNK), jnp.int32),
                pltpu.VMEM((hidden, f_in), BF16),
                pltpu.VMEM((rows_p, hidden), BF16),
                pltpu.VMEM((hidden, lanes_p), BF16),
                pltpu.VMEM((8, 1, LANES), F32),
                pltpu.VMEM((8, 1, LANES), F32),
                pltpu.VMEM((1, CHUNK), F32),
                pltpu.VMEM((8, f_in // 8, hidden), F32),
                pltpu.VMEM((8, f_in // 8, hidden), F32),
                pltpu.VMEM((8, f_in // 8, hidden), F32),
                pltpu.VMEM((2, 4, lanes_p // 8, hidden), F32),
                pltpu.VMEM((4, lanes_p // 8, hidden), F32),
                pltpu.VMEM((2, 4, lanes_p // 8, hidden), F32),
                pltpu.VMEM((4, lanes_p // 8, hidden), F32),
                pltpu.VMEM((3, lanes_p // 8, hidden), F32),
                dma((SLOTS, 2)), dma((CHUNKS,)), dma((4,)),
                dma((2, 4, CHUNKS)), dma((2, 4, CHUNKS)), dma((2, 4, CHUNKS)), dma((2, 4, CHUNKS)),
                dma((7,)), dma((7,)), dma((7,)), dma((7,)), dma((7,)), dma((7,)), dma((7,)), dma((7,)),
                dma((8,)), dma((8,)),
            ],
            compiler_params=pltpu.CompilerParams(
                collective_id=0, has_side_effects=True, vmem_limit_bytes=67_000_000),
        )(adj_rows, feat_rows.reshape(CHUNKS, CHUNK, f_in), w_one, w_two.T,
          label_rows.reshape(CHUNKS, 1, CHUNK), mask_rows.reshape(CHUNKS, 1, CHUNK))
        loss, dw1, dw2 = pl.pallas_call(
            output_kernel, name="outputs", in_specs=[vmem] * 3, out_specs=(vmem,) * 3,
            out_shape=tuple(jax.ShapeDtypeStruct(v.shape, v.dtype) for v in (loss, dw1, dw2)))(loss, dw1, dw2)
        return loss[0, 0], dw1, dw2.T

    return jax.shard_map(local_step, mesh=mesh, in_specs=(P(axis, None), P(axis, None), P(None, None), P(None, None), P(axis), P(axis)), out_specs=(P(), P(None, None), P(None, None)), check_vma=False)
```
